128 devices in a mesh: row: 16 (over x, y), col: 8 (over z, core).
Axes of the slice: x: 4, y: 4, z: 4, core: 2. Of those that a mesh axis runs over, the one named last changes fastest.
Arguments:
- tokens: bfloat16 [32, 8192], P(None, 'row'), may hold values from -6 to 6
- gain: float32 [8192], P('row'), may hold values from 0.24 to 4.5
- gate_weight: bfloat16 [8192, 28672], P('row', 'col'), may hold values from -0.0625 to 0.0625
- up_weight: bfloat16 [8192, 28672], P('row', 'col'), may hold values from -0.0625 to 0.0625
- down_weight: bfloat16 [28672, 8192], P('col', 'row'), may hold values from -0.03125 to 0.03125
- probes: float32 [4, 32, 8192], P(None, None, 'row'), may hold values from -6 to 6
Outputs:
- basis: float32 [4, 32, 8192], P(None, None, 'row')
- stretch: float32 [4], replicated
The draws below stay inside these ranges and needn't reach their ends.
All inputs are finite; a program needn't handle non-finite values.
Results may differ from the reference program's by a relative error of at most 0.0085.
Values may be sent and summed in bfloat16 or wider, within the bound.
A program may use at most 64 MiB of HBM per device.

```python
import jax
import jax.numpy as jnp
from jax import lax

D = 8192
FF = 28672
TOKENS = 32
PROBES = 4
ITERS = 3


def draw_gain(key, part):
    position = jnp.arange(D, dtype=jnp.float32) / max(D - 1, 1)
    jitter = jax.random.uniform(jax.random.fold_in(key, 11), (D,), jnp.float32, 0.8, 1.25)
    return 0.55 * jnp.power(3.0, position) * jitter


def levels(rng, extent, split, low, top_value):
    factor_of = 1.0
    for axis_at, shards_of in split:
        steps = jax.random.uniform(jax.random.fold_in(jax.random.fold_in(rng, 6), axis_at), (shards_of,), jnp.float32, low / len(split), top_value / len(split))
        factor_of = factor_of * jnp.repeat(jnp.exp(steps), extent[axis_at] // shards_of).reshape((-1,) + (1,) * (len(extent) - 1 - axis_at))
    return factor_of


def bell_draw(own_key, dims, deviation, most, cuts=(), held_as=jnp.bfloat16):
    result = deviation * jax.random.normal(own_key, dims, jnp.float32)
    if cuts:
        result = result * levels(own_key, dims, cuts, -0.22, 0.18)
    return jnp.clip(result, -most, most).astype(held_as)


def setup_inputs(seed: int = 0) -> dict:
    key_list = jax.random.split(jax.random.key(seed), 7)
    tokens = bell_draw(key_list[0], (TOKENS, D), 1.0, 6.0, ((1, 16),))
    gain = draw_gain(jax.random.fold_in(key_list[6], 71), 0)
    gate_weight = bell_draw(key_list[2], (D, FF), D ** -0.5, 0.0625, ((0, 16), (1, 8)))
    up_weight = bell_draw(key_list[3], (D, FF), D ** -0.5, 0.0625, ((0, 16), (1, 8)))
    down_weight = bell_draw(key_list[4], (FF, D), FF ** -0.5, 0.03125, ((0, 8), (1, 16)))
    probes = bell_draw(key_list[5], (PROBES, TOKENS, D), 1.0, 6.0, ((2, 16),), jnp.float32)
    return {"tokens": tokens, "gain": gain, "gate_weight": gate_weight, "up_weight": up_weight, "down_weight": down_weight, "probes": probes}


epsilon = 1e-06

def reference(tokens, gain, gate_weight, up_weight, down_weight, probes):
    scaled = (tokens.astype(jnp.float32) * gain).astype(jnp.bfloat16)
    gate = jnp.dot(scaled, gate_weight, preferred_element_type=jnp.float32)
    up = jnp.dot(scaled, up_weight, preferred_element_type=jnp.float32)
    sigmoid_gate = 1.0 / (1.0 + jnp.exp(-gate))
    activated = gate * sigmoid_gate
    slope = sigmoid_gate * (1.0 + gate * (1.0 - sigmoid_gate)) * up
    slope_all = jnp.tile(slope, (PROBES, 1))
    activated_all = jnp.tile(activated, (PROBES, 1))
    current = probes
    level = jnp.zeros((PROBES,), jnp.float32)
    for sweep in range(ITERS):
        pushed = (current * gain).astype(jnp.bfloat16).reshape(PROBES * TOKENS, D)
        gate_tan = jnp.dot(pushed, gate_weight, preferred_element_type=jnp.float32)
        up_tan = jnp.dot(pushed, up_weight, preferred_element_type=jnp.float32)
        hidden = (slope_all * gate_tan + activated_all * up_tan).astype(jnp.bfloat16)
        tangent = jnp.dot(hidden, down_weight, preferred_element_type=jnp.float32).astype(jnp.bfloat16)
        back = jnp.dot(tangent, down_weight.T, preferred_element_type=jnp.float32).astype(jnp.bfloat16)
        gate_pull = (slope_all * back).astype(jnp.bfloat16)
        up_pull = (activated_all * back).astype(jnp.bfloat16)
        pulled = jnp.dot(gate_pull, gate_weight.T, preferred_element_type=jnp.float32)
        pulled = pulled + jnp.dot(up_pull, up_weight.T, preferred_element_type=jnp.float32)
        grown = pulled.reshape(PROBES, TOKENS, D) * gain
        level = lax.optimization_barrier(jnp.mean(grown * grown, axis=(1, 2)))
        current = grown * lax.rsqrt(level + epsilon)[:, None, None]
    return (current, jnp.sqrt(level))
```

```python
import functools

import jax
import jax.numpy as jnp
from jax import lax
from jax.experimental import pallas as pl
from jax.experimental.pallas import tpu as pltpu
from jax.sharding import Mesh
from jax.sharding import PartitionSpec as P

ITERS = 3
EPSILON = 1e-06
MESH = pl.DeviceIdType.MESH
F32 = jnp.float32
BF16 = jnp.bfloat16
NT = (((1,), (1,)), ((), ()))
P2_TYPE = F32
HOP = 3.5
STEP = 0.7


def stage_order(chunks):
    events = []
    for k in range(chunks):
        begin = 2.0 + STEP * k
        events.append((0.3 * k, 0, k))
        for stage in range(1, 5):
            events.append((begin + HOP * stage, stage, k))
    return [(stage, k) for _, stage, k in sorted(events)]


def kernel(
    cfg,
    tokens_ref, gain_ref, gate_hbm, up_hbm, down_hbm, probes_ref,
    basis_ref, stretch_ref,
    gate_w, up_w, down_w,
    slope, act, pushed, tangent, grown_all, acc,
    joined, p1_src, p1_dst, p2_src, p2_dst, whole,
    t1_src, t1_dst, t2_src, t2_dst, t_whole,
    col_src, col_dst, sq1, sq1_in, sq2, scale,
    load_sem, p1_ss, p1_rs, p2_ss, p2_rs, g1_ss, g1_rs, g2_ss, g2_rs,
    col_ss, col_rs, ag_ss, ag_rs, sq1_ss, sq1_rs, sq2_ss, sq2_rs,
):
    N, NZ, NC, K, C, probe_count, token_count, entries = cfg
    G = NZ * NC
    M = probe_count * token_count
    R = M // N
    W = C // N
    RB = M // G
    width = gain_ref.shape[1]
    x, y, z, c = (lax.axis_index(name) for name in ("x", "y", "z", "c"))
    other = 1 - c
    a = x * other + y * c
    b = y * other + x * c
    g = z * NC + c

    def a_peer(d):
        return (lax.rem(x + d * other, N), lax.rem(y + d * c, N), z, c)

    def b_peer(d):
        return (lax.rem(x + d * c, N), lax.rem(y + d * other, N), z, c)

    def col_peer(dz, dc):
        return (x, y, lax.rem(z + dz, NZ), lax.rem(c + dc, NC))

    def plus(v, d, n):
        return lax.rem(v + d, n)

    row_offsets = [(dx, dy) for dx in range(N) for dy in range(N) if dx or dy]
    col_offsets = [(dz, dc) for dz in range(NZ) for dc in range(NC) if dz or dc]

    def remote(src, dst, send, recv, device):
        return pltpu.make_async_remote_copy(
            src_ref=src, dst_ref=dst, send_sem=send, recv_sem=recv,
            device_id=device, device_id_type=MESH,
        )

    loads = [
        pltpu.make_async_copy(hbm, vmem, load_sem.at[i])
        for i, (hbm, vmem) in enumerate(((gate_hbm, gate_w), (up_hbm, up_w), (down_hbm, down_w)))
    ]
    for load in loads:
        load.start()

    barrier = pltpu.get_barrier_semaphore()
    for dx, dy in row_offsets:
        device = (lax.rem(x + dx, N), lax.rem(y + dy, N), z, c)
        pl.semaphore_signal(barrier, inc=1, device_id=device, device_id_type=MESH)
    for dz, dc in col_offsets:
        pl.semaphore_signal(barrier, inc=1, device_id=col_peer(dz, dc), device_id_type=MESH)

    gain = gain_ref[...]
    pushed[...] = (
        (probes_ref[...] * gain[None]).astype(BF16).reshape(G, RB, width)
    )
    scaled = (tokens_ref[...].astype(F32) * gain).astype(BF16)
    scale[...] = jnp.ones_like(scale)

    pl.semaphore_wait(barrier, len(row_offsets) + len(col_offsets))
    loads[0].wait()
    loads[1].wait()

    def row_stages(part, own, src, dst, src2, dst2, gathered, emit, consume):
        def rs_a(k, d):
            return remote(
                src.at[k, plus(a, d, N)], dst.at[k, d - 1],
                p1_ss.at[k, d - 1], p1_rs.at[k, d - 1], a_peer(d),
            )

        def rs_b(k, d):
            return remote(
                src2.at[k, plus(b, d, N)], dst2.at[k, d - 1],
                p2_ss.at[k, d - 1], p2_rs.at[k, d - 1], b_peer(d),
            )

        def ag_b(k, d, sender):
            block = gathered.at[k, a, sender]
            return remote(block, block, g1_ss.at[k, d - 1], g1_rs.at[k, d - 1], b_peer(d))

        def ag_a(k, d, sender):
            block = gathered.at[k, sender]
            return remote(block, block, g2_ss.at[k, d - 1], g2_rs.at[k, d - 1], a_peer(d))

        far_first = sorted(range(1, N), key=lambda d: -min(d, N - d))

        def first(k):
            part(k)
            for d in far_first:
                rs_a(k, d).start()

        def second(k):
            total = own(k).astype(F32)
            for d in far_first[::-1]:
                rs_a(k, d).wait_recv()
                total += dst[k, d - 1].astype(F32)
            for j in range(N):
                src2[k, j] = total[:, j * W : (j + 1) * W].astype(src2.dtype)
            for d in far_first:
                rs_b(k, d).start()

        def third(k):
            total = src2[k, b].astype(F32)
            for d in far_first[::-1]:
                rs_b(k, d).wait_recv()
                total += dst2[k, d - 1].astype(F32)
            gathered[k, a, b] = emit(total).astype(gathered.dtype)
            for d in far_first:
                ag_b(k, d, b).start()

        def fourth(k):
            for d in far_first[::-1]:
                ag_b(k, d, plus(b, N - d, N)).wait_recv()
            for d in far_first:
                ag_a(k, d, a).start()

        def fifth(k):
            for d in far_first[::-1]:
                ag_a(k, d, plus(a, N - d, N)).wait_recv()
            consume(k)

        stages = (first, second, third, fourth, fifth)

        def finish():
            for k in range(K):
                for d in range(1, N):
                    rs_a(k, d).wait_send()
                    rs_b(k, d).wait_send()
                    ag_b(k, d, b).wait_send()
                    ag_a(k, d, a).wait_send()

        return stages, finish

    def run_stages(stages, finish, before_third=None):
        waiting = before_third
        for stage, k in stage_order(K):
            if stage == 2 and waiting is not None:
                waiting()
                waiting = None
            stages[stage](k)
        finish()

    def columns(k):
        return slice(k * C, (k + 1) * C)

    half = N // 2

    def token_part(k):
        gate = jnp.dot(scaled, gate_w[:, columns(k)], preferred_element_type=F32)
        up = jnp.dot(scaled, up_w[:, columns(k)], preferred_element_type=F32)
        t1_src[k, :half] = gate.reshape(half, token_count // half, C)
        t1_src[k, half:] = up.reshape(half, token_count // half, C)

    def token_values(k, lo):
        return jnp.concatenate(
            [
                jnp.concatenate([t_whole[k, i, j] for i in range(lo, lo + half)], axis=0)
                for j in range(N)
            ],
            axis=1,
        )

    def token_use(k):
        gate = token_values(k, 0)
        up = token_values(k, half)
        sigmoid = 1.0 / (1.0 + jnp.exp(-gate))
        act[:, columns(k)] = gate * sigmoid
        slope[:, columns(k)] = sigmoid * (1.0 + gate * (1.0 - sigmoid)) * up

    run_stages(
        *row_stages(
            token_part, lambda k: t1_src[k, a], t1_src, t1_dst, t2_src, t2_dst, t_whole,
            lambda total: total, token_use,
        )
    )
    loads[2].wait()

    def by_token(values, factor):
        return (values.reshape(probe_count, token_count, C) * factor[None]).reshape(M, C)

    def send_joined(k, value):
        blocks = value.reshape(N, R, C)
        joined[k] = blocks
        p1_src[k] = blocks.astype(BF16)

    def chunk_rows(k):
        return jnp.concatenate(
            [whole[k, :, j].reshape(M, W) for j in range(N)], axis=1
        )

    def hidden_part(k):
        lhs = pushed[...].reshape(M, width)
        gate_tan = jnp.dot(lhs, gate_w[:, columns(k)], preferred_element_type=F32)
        up_tan = jnp.dot(lhs, up_w[:, columns(k)], preferred_element_type=F32)
        send_joined(k, by_token(gate_tan, slope[:, columns(k)]) + by_token(up_tan, act[:, columns(k)]))

    def add_to_acc(k, value):
        acc[...] = value if k == 0 else acc[...] + value

    def hidden_use(k):
        add_to_acc(k, jnp.dot(chunk_rows(k), down_w[columns(k), :], preferred_element_type=F32))

    def back_part(k):
        lhs = tangent[...].reshape(M, width)
        send_joined(k, lax.dot_general(lhs, down_w[columns(k), :], NT, preferred_element_type=F32))

    def back_use(k):
        piece = chunk_rows(k).astype(F32)
        gate_pull = by_token(piece, slope[:, columns(k)]).astype(BF16)
        up_pull = by_token(piece, act[:, columns(k)]).astype(BF16)
        value = lax.dot_general(gate_pull, gate_w[:, columns(k)], NT, preferred_element_type=F32)
        value += lax.dot_general(up_pull, up_w[:, columns(k)], NT, preferred_element_type=F32)
        add_to_acc(k, value)

    def col_index(dz, dc):
        return lax.rem(z + dz, NZ) * NC + lax.rem(c + dc, NC)

    def col_from(dz, dc):
        return lax.rem(z + NZ - dz, NZ) * NC + lax.rem(c + NC - dc, NC)

    def col_reduced(which):
        col_src[which] = acc[...].reshape(G, RB, width)

        def copy(slot, dz, dc):
            return remote(
                col_src.at[which, col_index(dz, dc)], col_dst.at[which, slot],
                col_ss.at[which, slot], col_rs.at[which, slot], col_peer(dz, dc),
            )

        copies = [copy(slot, dz, dc) for slot, (dz, dc) in enumerate(col_offsets)]
        for cp in copies[::-1]:
            cp.start()
        total = col_src[which, g]
        for slot, cp in enumerate(copies):
            cp.wait_recv()
            total += col_dst[which, slot]
        for cp in copies:
            cp.wait_send()
        return total

    def col_gather(buffer, sems):
        send, recv = ag_ss.at[sems], ag_rs.at[sems]

        def copy(slot, dz, dc, owner):
            return remote(buffer.at[owner], buffer.at[owner], send.at[slot], recv.at[slot], col_peer(dz, dc))

        for slot, (dz, dc) in reversed(list(enumerate(col_offsets))):
            copy(slot, dz, dc, g).start()

        def finish():
            for slot, (dz, dc) in enumerate(col_offsets):
                copy(slot, dz, dc, col_from(dz, dc)).wait_recv()
            for slot, (dz, dc) in enumerate(col_offsets):
                copy(slot, dz, dc, g).wait_send()

        return finish

    def fold(values):
        rows, lanes = values.shape
        total = None
        for r in range(0, rows, 8):
            for l in range(0, lanes, 128):
                piece = values[r : r + 8, l : l + 128]
                total = piece if total is None else total + piece
        return total

    def square_copies():
        return [
            remote(
                sq1, sq1_in.at[slot], sq1_ss.at[slot], sq1_rs.at[slot],
                (lax.rem(x + dx, N), lax.rem(y + dy, N), z, c),
            )
            for slot, (dx, dy) in enumerate(row_offsets)
        ]

    def level_copy(slot, dz, dc, owner):
        return remote(sq2.at[owner], sq2.at[owner], sq2_ss.at[slot], sq2_rs.at[slot], col_peer(dz, dc))

    def squares_over_row():
        copies = square_copies()
        total = sq1[...]
        for slot, cp in enumerate(copies):
            cp.wait_recv()
            total += sq1_in[slot]
        for cp in copies:
            cp.wait_send()
        sq2[g] = total
        for slot, (dz, dc) in reversed(list(enumerate(col_offsets))):
            level_copy(slot, dz, dc, g).start()

    def squares_over_col():
        for slot, (dz, dc) in enumerate(col_offsets):
            level_copy(slot, dz, dc, col_from(dz, dc)).wait_recv()
            level_copy(slot, dz, dc, g).wait_send()

    owners = token_count // RB

    def level_of(probe):
        total = sq2[probe * owners]
        for i in range(1, owners):
            total += sq2[probe * owners + i]
        return jnp.sum(jnp.sum(total, axis=0, keepdims=True), axis=1, keepdims=True) / entries

    def sweep(it, carry):
        def norms():
            @pl.when(it > 0)
            def _():
                squares_over_row()

        run_stages(
            *row_stages(
                hidden_part, lambda k: joined[k, a], p1_src, p1_dst, p2_src, p2_dst, whole,
                lambda total: total, hidden_use,
            ),
            before_third=norms,
        )

        @pl.when(it > 0)
        def _():
            squares_over_col()
            factor = lax.rsqrt(level_of(g // owners) + EPSILON)
            scale[...] = jnp.broadcast_to(factor, scale.shape)

        total = col_reduced(0)
        tangent[g] = (total * scale[0:1, 0:1]).astype(BF16)
        col_gather(tangent, 0)()

        run_stages(
            *row_stages(
                back_part, lambda k: joined[k, a], p1_src, p1_dst, p2_src, p2_dst, whole,
                lambda total: total, back_use,
            )
        )
        grown = col_reduced(1) * gain
        grown_all[g] = grown
        sq1[...] = fold(grown * grown)
        for cp in square_copies():
            cp.start()

        @pl.when(it < ITERS - 1)
        def _():
            pushed[g] = (grown * gain).astype(BF16)
            col_gather(pushed, 1)()

        return carry

    lax.fori_loop(0, ITERS, sweep, 0)

    wait_grown = col_gather(grown_all, 2)
    squares_over_row()
    wait_grown()
    squares_over_col()
    lane = lax.broadcasted_iota(jnp.int32, (1, probe_count), 1)
    stretch = jnp.zeros((1, probe_count), F32)
    per = G // probe_count
    for p in range(probe_count):
        level = level_of(p)
        stretch = jnp.where(lane == p, jnp.sqrt(level), stretch)
        rows = jnp.concatenate([grown_all[p * per + i] for i in range(per)], axis=0)
        basis_ref[p] = rows * lax.rsqrt(level + EPSILON)
    stretch_ref[...] = stretch


def solution(mesh, chunk=512, shape=(4, 4, 4, 2)):
    N, _, NZ, NC = shape
    torus = Mesh(mesh.devices.reshape(shape), ("x", "y", "z", "c"))
    row, col = ("x", "y"), ("z", "c")

    def local(tokens, gain, gate_weight, up_weight, down_weight, probes):
        probe_count, token_count, width = probes.shape
        hidden = gate_weight.shape[1]
        M = probe_count * token_count
        G = NZ * NC
        K, C = hidden // chunk, chunk
        R, W, RB = M // N, C // N, M // G
        TR = 2 * token_count // N
        entries = token_count * width * N * N
        cfg = (N, NZ, NC, K, C, probe_count, token_count, entries)
        vm = pltpu.VMEM
        dma = pltpu.SemaphoreType.DMA
        basis, stretch = pl.pallas_call(
            functools.partial(kernel, cfg),
            out_shape=(
                jax.ShapeDtypeStruct(probes.shape, F32),
                jax.ShapeDtypeStruct((1, probe_count), F32),
            ),
            in_specs=[
                pl.BlockSpec(memory_space=pltpu.VMEM),
                pl.BlockSpec(memory_space=pltpu.VMEM),
                pl.BlockSpec(memory_space=pl.ANY),
                pl.BlockSpec(memory_space=pl.ANY),
                pl.BlockSpec(memory_space=pl.ANY),
                pl.BlockSpec(memory_space=pltpu.VMEM),
            ],
            out_specs=(
                pl.BlockSpec(memory_space=pltpu.VMEM),
                pl.BlockSpec(memory_space=pltpu.VMEM),
            ),
            scratch_shapes=[
                vm((width, hidden), BF16), vm((width, hidden), BF16), vm((hidden, width), BF16),
                vm((token_count, hidden), F32), vm((token_count, hidden), F32),
                vm((G, RB, width), BF16), vm((G, RB, width), BF16), vm((G, RB, width), F32),
                vm((M, width), F32),
                vm((K, N, R, C), F32), vm((K, N, R, C), BF16), vm((K, N - 1, R, C), BF16),
                vm((K, N, R, W), P2_TYPE), vm((K, N - 1, R, W), P2_TYPE), vm((K, N, N, R, W), BF16),
                vm((K, N, TR, C), F32), vm((K, N - 1, TR, C), F32),
                vm((K, N, TR, W), F32), vm((K, N - 1, TR, W), F32), vm((K, N, N, TR, W), F32),
                vm((2, G, RB, width), F32), vm((2, G - 1, RB, width), F32),
                vm((8, 128), F32), vm((N * N - 1, 8, 128), F32), vm((G, 8, 128), F32),
                vm((8, 128), F32),
                dma((3,)),
                *[dma((K, N - 1)) for _ in range(8)],
                dma((2, G - 1)), dma((2, G - 1)),
                dma((3, G - 1)), dma((3, G - 1)),
                dma((N * N - 1,)), dma((N * N - 1,)),
                dma((G - 1,)), dma((G - 1,)),
            ],
            compiler_params=pltpu.CompilerParams(collective_id=0, has_side_effects=True),
        )(tokens, gain.reshape(1, width), gate_weight, up_weight, down_weight, probes)
        return basis, stretch.reshape(probe_count)

    return jax.shard_map(
        local,
        mesh=torus,
        in_specs=(P(None, row), P(row), P(row, col), P(row, col), P(col, row), P(None, None, row)),
        out_specs=(P(None, None, row), P()),
        check_vma=False,
    )
```

```python
import functools

import jax
import jax.numpy as jnp
from jax import lax
from jax.experimental import pallas as pl
from jax.experimental.pallas import tpu as pltpu
from jax.sharding import Mesh
from jax.sharding import PartitionSpec as P

ITERS = 3
EPSILON = 1e-06
MESH = pl.DeviceIdType.MESH
F32 = jnp.float32
BF16 = jnp.bfloat16
NT = (((1,), (1,)), ((), ()))
CHUNK = 512
MODES = (3, 3, 3, 3, 3, 3, 3)
TOKEN_MODES = (3, 3, 3, 3, 3, 3, 3)
TOKEN_TYPES = (BF16, F32, F32)
HOP = 3.0
STEP = 0.8


def stage_order(modes):
    events = []
    for k, mode in enumerate(modes):
        events.append((0.3 * k, 0, k))
        for stage in range(1, mode + 1):
            events.append((1.0 + STEP * (k + 1) + HOP * stage, stage, k))
    return [(stage, k) for _, stage, k in sorted(events)]


def kernel(
    cfg,
    tokens_ref, gain_ref, gate_hbm, up_hbm, down_hbm, probes_ref,
    basis_ref, stretch_ref,
    gate_w, up_w, down_w,
    slope, act, pushed, tangent, grown_all, acc,
    joined, p1_src, p1_dst, p2_src, p2_dst, whole,
    t1_own, t1_src, t1_dst, t2_src, t2_dst, t_whole,
    pair_in, z_src, z_dst, sq, sq_in, scale,
    gate_sem, up_sem, down_sem, p1_ss, p1_rs, p2_ss, p2_rs, g1_ss, g1_rs, g2_ss, g2_rs,
    pair_ss, pair_rs, z_ss, z_rs, sq_ss, sq_rs,
):
    N, NZ, K, C, probe_count, token_count, entries = cfg
    M = probe_count * token_count
    R = M // N
    W = C // N
    half = M // 2
    half_probes = probe_count // 2
    width = gain_ref.shape[1]
    x, y, z, c = (lax.axis_index(name) for name in ("x", "y", "z", "c"))
    other = 1 - c
    a = x * other + y * c
    b = y * other + x * c

    def a_peer(d):
        return (lax.rem(x + d * other, N), lax.rem(y + d * c, N), z, c)

    def b_peer(d):
        return (lax.rem(x + d * c, N), lax.rem(y + d * other, N), z, c)

    def row_peer(dx, dy):
        return (lax.rem(x + dx, N), lax.rem(y + dy, N), z, c)

    def z_peer(d):
        return (x, y, lax.rem(z + d, NZ), c)

    partner = (x, y, z, other)
    row_offsets = [(dx, dy) for dx in range(N) for dy in range(N) if dx or dy]

    def plus(v, d, n):
        return lax.rem(v + d, n)

    def columns(k):
        return slice(k * C, (k + 1) * C)

    def remote(src, dst, send, recv, device):
        return pltpu.make_async_remote_copy(
            src_ref=src, dst_ref=dst, send_sem=send, recv_sem=recv,
            device_id=device, device_id_type=MESH,
        )

    gate_loads = [
        pltpu.make_async_copy(gate_hbm.at[:, columns(k)], gate_w.at[:, columns(k)], gate_sem.at[k])
        for k in range(K)
    ]
    up_loads = [
        pltpu.make_async_copy(up_hbm.at[:, columns(k)], up_w.at[:, columns(k)], up_sem.at[k])
        for k in range(K)
    ]
    down_load = pltpu.make_async_copy(down_hbm, down_w, down_sem.at[0])
    for k in range(K):
        gate_loads[k].start()
        up_loads[k].start()
    down_load.start()

    barrier = pltpu.get_barrier_semaphore()
    greeted = [row_peer(dx, dy) for dx, dy in row_offsets]
    greeted += [z_peer(d) for d in range(1, NZ)] + [partner]
    for device in greeted:
        pl.semaphore_signal(barrier, inc=1, device_id=device, device_id_type=MESH)

    gain = gain_ref[...]
    pushed[...] = (probes_ref[...] * gain[None]).astype(BF16).reshape(2, half, width)
    scaled = (tokens_ref[...].astype(F32) * gain).astype(BF16)
    scale[...] = jnp.ones_like(scale)

    far_first = sorted(range(1, N), key=lambda d: -min(d, N - d))
    near_first = far_first[::-1]

    def row_stages(phase, part, own, modes, src, dst, src2, dst2, gathered, consume):
        def block(j):
            return pl.ds(pl.multiple_of(j * W, W), W)

        def rs_a(k, d):
            return remote(
                src.at[k, plus(a, d, N)], dst.at[k, d - 1],
                p1_ss.at[k, d - 1], p1_rs.at[k, d - 1], a_peer(d),
            )

        def over_b(k, d):
            if modes[k] == 3:
                sent, taken = src2.at[k], dst2.at[k, d - 1]
            else:
                sent, taken = src2.at[k, :, block(plus(b, d, N))], dst2.at[k, d - 1, :, 0:W]
            return remote(sent, taken, p2_ss.at[phase, k, d - 1], p2_rs.at[phase, k, d - 1], b_peer(d))

        def ag_b(k, d, sender):
            piece = gathered.at[k, a, :, block(sender)]
            return remote(piece, piece, g1_ss.at[k, d - 1], g1_rs.at[k, d - 1], b_peer(d))

        def ag_a(k, d, sender):
            piece = gathered.at[k, sender]
            return remote(piece, piece, g2_ss.at[k, d - 1], g2_rs.at[k, d - 1], a_peer(d))

        def first(k):
            part(k)
            for d in far_first:
                rs_a(k, d).start()

        def second(k):
            total = own(k)
            for d in near_first:
                rs_a(k, d).wait_recv()
                total += dst[k, d - 1].astype(F32)
            src2[k] = total.astype(src2.dtype)
            for d in far_first:
                over_b(k, d).start()
            own_sum(k, total)

        def own_sum(k, total):
            kept = joined if src is p1_src else t1_own
            kept[k, a] = total

        def third(k):
            kept = joined if src is p1_src else t1_own
            if modes[k] == 3:
                total = kept[k, a]
                for d in near_first:
                    over_b(k, d).wait_recv()
                    total += dst2[k, d - 1].astype(F32)
                gathered[k, a] = total.astype(gathered.dtype)
                for d in far_first:
                    ag_a(k, d, a).start()
            else:
                total = kept[k, a, :, block(b)]
                for d in near_first:
                    over_b(k, d).wait_recv()
                    total += dst2[k, d - 1, :, 0:W].astype(F32)
                gathered[k, a, :, block(b)] = total.astype(gathered.dtype)
                for d in far_first:
                    ag_b(k, d, b).start()

        def fourth(k):
            for d in near_first:
                ag_b(k, d, plus(b, N - d, N)).wait_recv()
            for d in far_first:
                ag_a(k, d, a).start()

        def last(k):
            for d in near_first:
                ag_a(k, d, plus(a, N - d, N)).wait_recv()
            consume(k)

        def stages_of(k):
            return (first, second, third, last) if modes[k] == 3 else (first, second, third, fourth, last)

        def finish():
            for k in range(K):
                for d in range(1, N):
                    rs_a(k, d).wait_send()
                    over_b(k, d).wait_send()
                    if modes[k] == 4:
                        ag_b(k, d, b).wait_send()
                    ag_a(k, d, a).wait_send()

        for stage, k in stage_order(modes):
            stages_of(k)[stage](k)
        finish()

    halves = N // 2

    def token_compute(k):
        gate_loads[k].wait()
        up_loads[k].wait()
        gate = jnp.dot(scaled, gate_w[:, columns(k)], preferred_element_type=F32)
        up = jnp.dot(scaled, up_w[:, columns(k)], preferred_element_type=F32)
        gate = gate.reshape(halves, token_count // halves, C)
        up = up.reshape(halves, token_count // halves, C)
        t1_own[k, :halves] = gate
        t1_own[k, halves:] = up
        t1_src[k, :halves] = gate.astype(t1_src.dtype)
        t1_src[k, halves:] = up.astype(t1_src.dtype)

    for k in range(K):
        token_compute(k)
    pl.semaphore_wait(barrier, len(greeted))

    def token_use(k):
        gate = t_whole[k, :halves].reshape(token_count, C).astype(F32)
        up = t_whole[k, halves:].reshape(token_count, C).astype(F32)
        sigmoid = 1.0 / (1.0 + jnp.exp(-gate))
        act[:, columns(k)] = gate * sigmoid
        slope[:, columns(k)] = sigmoid * (1.0 + gate * (1.0 - sigmoid)) * up

    row_stages(
        2, lambda k: None, lambda k: t1_own[k, a], TOKEN_MODES,
        t1_src, t1_dst, t2_src, t2_dst, t_whole, token_use,
    )
    down_load.wait()

    def by_token(values, factor):
        return (values.reshape(probe_count, token_count, C) * factor[None]).reshape(M, C)

    def send_joined(k, value):
        blocks = value.reshape(N, R, C)
        joined[k] = blocks
        p1_src[k] = blocks.astype(BF16)

    def hidden_part(k):
        lhs = pushed[...].reshape(M, width)
        gate_tan = jnp.dot(lhs, gate_w[:, columns(k)], preferred_element_type=F32)
        up_tan = jnp.dot(lhs, up_w[:, columns(k)], preferred_element_type=F32)
        send_joined(k, by_token(gate_tan, slope[:, columns(k)]) + by_token(up_tan, act[:, columns(k)]))

    def add_to_acc(k, value):
        value = value.reshape(2, half, width)
        acc[...] = value if k == 0 else acc[...] + value

    def hidden_use(k):
        lhs = whole[k].reshape(M, C)
        add_to_acc(k, jnp.dot(lhs, down_w[columns(k), :], preferred_element_type=F32))

    def back_part(k):
        lhs = tangent[...].reshape(M, width)
        send_joined(k, lax.dot_general(lhs, down_w[columns(k), :], NT, preferred_element_type=F32))

    def back_use(k):
        piece = whole[k].reshape(M, C).astype(F32)
        gate_pull = by_token(piece, slope[:, columns(k)]).astype(BF16)
        up_pull = by_token(piece, act[:, columns(k)]).astype(BF16)
        value = lax.dot_general(gate_pull, gate_w[:, columns(k)], NT, preferred_element_type=F32)
        value += lax.dot_general(up_pull, up_w[:, columns(k)], NT, preferred_element_type=F32)
        add_to_acc(k, value)

    def col_half(phase):
        swap = remote(acc.at[other], pair_in, pair_ss.at[0], pair_rs.at[0], partner)
        swap.start()
        total = acc[c]
        swap.wait_recv()
        total += pair_in[...]
        z_src[...] = total.astype(z_src.dtype)
        copies = [
            remote(z_src, z_dst.at[phase, d - 1], z_ss.at[phase, d - 1], z_rs.at[phase, d - 1], z_peer(d))
            for d in range(1, NZ)
        ]
        for d in sorted(range(1, NZ), key=lambda d: -min(d, NZ - d)):
            copies[d - 1].start()
        acc[c] = total
        swap.wait_send()
        for d in sorted(range(1, NZ), key=lambda d: min(d, NZ - d)):
            copies[d - 1].wait_recv()
        total = acc[c]
        for d in range(1, NZ):
            total += z_dst[phase, d - 1].astype(F32)
        for cp in copies:
            cp.wait_send()
        return total

    def share(buffer, which):
        mine, theirs = buffer.at[c], buffer.at[other]
        send, recv = pair_ss.at[which], pair_rs.at[which]
        remote(mine, mine, send, recv, partner).start()
        remote(theirs, theirs, send, recv, partner).wait_recv()
        remote(mine, mine, send, recv, partner).wait_send()

    def folded(values):
        rows, lanes = values.shape
        total = None
        for r in range(0, rows, 8):
            for l in range(0, lanes, 128):
                piece = values[r : r + 8, l : l + 128]
                total = piece if total is None else total + piece
        return jnp.sum(total, axis=0, keepdims=True)

    def square_copies():
        return [
            remote(sq, sq_in.at[slot], sq_ss.at[slot], sq_rs.at[slot], row_peer(dx, dy))
            for slot, (dx, dy) in enumerate(row_offsets)
        ]

    def send_squares():
        for p in range(probe_count):
            i, j = divmod(p, half_probes)
            values = grown_all[i, j * token_count : (j + 1) * token_count]
            sq[p : p + 1] = folded(values * values)
        for cp in square_copies():
            cp.start()

    def levels():
        total = sq[...]
        copies = square_copies()
        for cp in copies:
            cp.wait_recv()
        for slot in range(len(copies)):
            total += sq_in[slot]
        for cp in copies:
            cp.wait_send()
        return jnp.sum(total, axis=1, keepdims=True) / entries

    def sweep(it, carry):
        row_stages(
            0, hidden_part, lambda k: joined[k, a], MODES, p1_src, p1_dst, p2_src, p2_dst.at[0], whole, hidden_use,
        )
        total = col_half(0)

        @pl.when(it > 0)
        def _():
            factor = lax.rsqrt(levels() + EPSILON)
            for p in range(probe_count):
                scale[p] = jnp.broadcast_to(factor[p : p + 1], scale.shape[1:])

        parts = [
            total[i * token_count : (i + 1) * token_count] * scale[c * half_probes + i, 0:1, 0:1]
            for i in range(half_probes)
        ]
        tangent[c] = jnp.concatenate(parts, axis=0).astype(BF16)
        share(tangent, 1)

        row_stages(
            1, back_part, lambda k: joined[k, a], MODES, p1_src, p1_dst, p2_src, p2_dst.at[1], whole, back_use,
        )
        grown_all[c] = col_half(1) * gain
        share(grown_all, 2)
        send_squares()
        pushed[...] = (grown_all[...] * gain[None]).astype(BF16)
        return carry

    sq[...] = jnp.zeros_like(sq)
    lax.fori_loop(0, ITERS, sweep, 0)

    level = levels()
    root = jnp.sqrt(level)
    factor = lax.rsqrt(level + EPSILON)
    lane = lax.broadcasted_iota(jnp.int32, (1, probe_count), 1)
    stretch = jnp.zeros((1, probe_count), F32)
    for p in range(probe_count):
        stretch = jnp.where(lane == p, root[p : p + 1], stretch)
        i, j = divmod(p, half_probes)
        basis_ref[p] = grown_all[i, j * token_count : (j + 1) * token_count] * factor[p : p + 1]
    stretch_ref[...] = stretch


def solution(mesh, chunk=CHUNK, shape=(4, 4, 4, 2)):
    N, _, NZ, _ = shape
    torus = Mesh(mesh.devices.reshape(shape), ("x", "y", "z", "c"))
    row, col = ("x", "y"), ("z", "c")

    def local(tokens, gain, gate_weight, up_weight, down_weight, probes):
        probe_count, token_count, width = probes.shape
        hidden = gate_weight.shape[1]
        M = probe_count * token_count
        K, C = hidden // chunk, chunk
        R = M // N
        TR = 2 * token_count // N
        T1, T2, TG = TOKEN_TYPES
        entries = token_count * width * N * N
        cfg = (N, NZ, K, C, probe_count, token_count, entries)
        vm = pltpu.VMEM
        dma = pltpu.SemaphoreType.DMA
        basis, stretch = pl.pallas_call(
            functools.partial(kernel, cfg),
            out_shape=(
                jax.ShapeDtypeStruct(probes.shape, F32),
                jax.ShapeDtypeStruct((1, probe_count), F32),
            ),
            in_specs=[
                pl.BlockSpec(memory_space=pltpu.VMEM),
                pl.BlockSpec(memory_space=pltpu.VMEM),
                pl.BlockSpec(memory_space=pl.ANY),
                pl.BlockSpec(memory_space=pl.ANY),
                pl.BlockSpec(memory_space=pl.ANY),
                pl.BlockSpec(memory_space=pltpu.VMEM),
            ],
            out_specs=(
                pl.BlockSpec(memory_space=pltpu.VMEM),
                pl.BlockSpec(memory_space=pltpu.VMEM),
            ),
            scratch_shapes=[
                vm((width, hidden), BF16), vm((width, hidden), BF16), vm((hidden, width), BF16),
                vm((token_count, hidden), F32), vm((token_count, hidden), F32),
                vm((2, M // 2, width), BF16), vm((2, M // 2, width), BF16), vm((2, M // 2, width), F32),
                vm((2, M // 2, width), F32),
                vm((K, N, R, C), F32), vm((K, N, R, C), BF16), vm((K, N - 1, R, C), BF16),
                vm((K, R, C), BF16), vm((2, K, N - 1, R, C), BF16), vm((K, N, R, C), BF16),
                vm((K, N, TR, C), F32), vm((K, N, TR, C), T1), vm((K, N - 1, TR, C), T1),
                vm((K, TR, C), T2), vm((K, N - 1, TR, C), T2), vm((K, N, TR, C), TG),
                vm((M // 2, width), F32), vm((M // 2, width), BF16), vm((2, NZ - 1, M // 2, width), BF16),
                vm((8, 128), F32), vm((N * N - 1, 8, 128), F32),
                vm((probe_count, 8, 128), F32),
                dma((K,)), dma((K,)), dma((1,)),
                dma((K, N - 1)), dma((K, N - 1)), dma((3, K, N - 1)), dma((3, K, N - 1)),
                *[dma((K, N - 1)) for _ in range(4)],
                dma((3,)), dma((3,)),
                dma((2, NZ - 1)), dma((2, NZ - 1)),
                dma((N * N - 1,)), dma((N * N - 1,)),
            ],
            compiler_params=pltpu.CompilerParams(collective_id=0, has_side_effects=True),
        )(tokens, gain.reshape(1, width), gate_weight, up_weight, down_weight, probes)
        return basis, stretch.reshape(probe_count)

    return jax.shard_map(
        local,
        mesh=torus,
        in_specs=(P(None, row), P(row), P(row, col), P(row, col), P(col, row), P(None, None, row)),
        out_specs=(P(None, None, row), P()),
        check_vma=False,
    )
```

```python
import functools

import jax
import jax.numpy as jnp
from jax import lax
from jax.experimental import pallas as pl
from jax.experimental.pallas import tpu as pltpu
from jax.sharding import Mesh
from jax.sharding import PartitionSpec as P

ITERS = 3
EPSILON = 1e-06
MESH = pl.DeviceIdType.MESH
F32 = jnp.float32
BF16 = jnp.bfloat16
NT = (((1,), (1,)), ((), ()))
CHUNK = 512
MODES = (3, 3, 3, 3, 3, 3, 3)
TOKEN_MODES = (3, 3, 3, 3, 3, 3, 3)
TOKEN_TYPES = (BF16, F32, F32)
HOP = 3.0
STEP = 0.5


def stage_order(modes):
    events = []
    for k, mode in enumerate(modes):
        events.append((0.3 * k, 0, k))
        for stage in range(1, mode + 1):
            events.append((1.0 + STEP * (k + 1) + HOP * stage, stage, k))
    return [(stage, k) for _, stage, k in sorted(events)]


def kernel(
    cfg,
    tokens_ref, gain_ref, gate_hbm, up_hbm, down_hbm, probes_ref,
    basis_ref, stretch_ref,
    gate_w, up_w, down_w,
    slope, act, pushed, tangent, grown_all, acc,
    joined, p1_src, p1_dst, p2_src, p2_dst, whole,
    t1_own, t1_src, t1_dst, t2_src, t2_dst, t_whole,
    pair_in, z_src, z_dst, sq, sq_in, scale,
    gate_sem, up_sem, down_sem, p1_ss, p1_rs, p2_ss, p2_rs, g1_ss, g1_rs, g2_ss, g2_rs,
    pair_ss, pair_rs, z_ss, z_rs, sq_ss, sq_rs,
):
    N, NZ, K, C, probe_count, token_count, entries = cfg
    M = probe_count * token_count
    R = M // N
    W = C // N
    half = M // 2
    half_probes = probe_count // 2
    width = gain_ref.shape[1]
    x, y, z, c = (lax.axis_index(name) for name in ("x", "y", "z", "c"))
    other = 1 - c
    swaps = (c, other)
    a_at = (x * other + y * c, y * other + x * c)

    def a_of(k):
        return a_at[k % 2]

    def b_of(k):
        return a_at[1 - k % 2]

    def a_peer(k, d):
        swap = swaps[k % 2]
        return (lax.rem(x + d * (1 - swap), N), lax.rem(y + d * swap, N), z, c)

    def b_peer(k, d):
        return a_peer(k + 1, d)

    def row_peer(dx, dy):
        return (lax.rem(x + dx, N), lax.rem(y + dy, N), z, c)

    def z_peer(d):
        return (x, y, lax.rem(z + d, NZ), c)

    partner = (x, y, z, other)
    row_offsets = [(dx, dy) for dx in range(N) for dy in range(N) if dx or dy]

    def plus(v, d, n):
        return lax.rem(v + d, n)

    def columns(k):
        return slice(k * C, (k + 1) * C)

    def remote(src, dst, send, recv, device):
        return pltpu.make_async_remote_copy(
            src_ref=src, dst_ref=dst, send_sem=send, recv_sem=recv,
            device_id=device, device_id_type=MESH,
        )

    gate_loads = [
        pltpu.make_async_copy(gate_hbm.at[:, columns(k)], gate_w.at[:, columns(k)], gate_sem.at[k])
        for k in range(K)
    ]
    up_loads = [
        pltpu.make_async_copy(up_hbm.at[:, columns(k)], up_w.at[:, columns(k)], up_sem.at[k])
        for k in range(K)
    ]
    down_load = pltpu.make_async_copy(down_hbm, down_w, down_sem.at[0])
    for k in range(K):
        gate_loads[k].start()
        up_loads[k].start()
    down_load.start()

    barrier = pltpu.get_barrier_semaphore()
    greeted = [row_peer(dx, dy) for dx, dy in row_offsets]
    greeted += [z_peer(d) for d in range(1, NZ)] + [partner]
    for device in greeted:
        pl.semaphore_signal(barrier, inc=1, device_id=device, device_id_type=MESH)

    gain = gain_ref[...]
    pushed[...] = (probes_ref[...] * gain[None]).astype(BF16).reshape(2, half, width)
    scaled = (tokens_ref[...].astype(F32) * gain).astype(BF16)
    scale[...] = jnp.ones_like(scale)

    far_first = sorted(range(1, N), key=lambda d: -min(d, N - d))
    near_first = far_first[::-1]

    def row_stages(phase, part, own, modes, src, dst, src2, dst2, gathered, consume):
        def block(j):
            return pl.ds(pl.multiple_of(j * W, W), W)

        def rs_a(k, d):
            return remote(
                src.at[k, plus(a_of(k), d, N)], dst.at[k, d - 1],
                p1_ss.at[k, d - 1], p1_rs.at[k, d - 1], a_peer(k, d),
            )

        def over_b(k, d):
            if modes[k] == 3:
                sent, taken = src2.at[k], dst2.at[k, d - 1]
            else:
                sent, taken = src2.at[k, :, block(plus(b_of(k), d, N))], dst2.at[k, d - 1, :, 0:W]
            return remote(sent, taken, p2_ss.at[phase, k, d - 1], p2_rs.at[phase, k, d - 1], b_peer(k, d))

        def ag_b(k, d, sender):
            piece = gathered.at[k, a_of(k), :, block(sender)]
            return remote(piece, piece, g1_ss.at[k, d - 1], g1_rs.at[k, d - 1], b_peer(k, d))

        def ag_a(k, d, sender):
            piece = gathered.at[k, sender]
            return remote(piece, piece, g2_ss.at[k, d - 1], g2_rs.at[k, d - 1], a_peer(k, d))

        def first(k):
            part(k)
            for d in far_first:
                rs_a(k, d).start()

        def second(k):
            total = own(k)
            for d in near_first:
                rs_a(k, d).wait_recv()
                total += dst[k, d - 1].astype(F32)
            src2[k] = total.astype(src2.dtype)
            for d in far_first:
                over_b(k, d).start()
            own_sum(k, total)

        def own_sum(k, total):
            kept = joined if src is p1_src else t1_own
            kept[k, a_of(k)] = total

        def third(k):
            kept = joined if src is p1_src else t1_own
            if modes[k] == 3:
                total = kept[k, a_of(k)]
                for d in near_first:
                    over_b(k, d).wait_recv()
                    total += dst2[k, d - 1].astype(F32)
                gathered[k, a_of(k)] = total.astype(gathered.dtype)
                for d in far_first:
                    ag_a(k, d, a_of(k)).start()
            else:
                total = kept[k, a_of(k), :, block(b_of(k))]
                for d in near_first:
                    over_b(k, d).wait_recv()
                    total += dst2[k, d - 1, :, 0:W].astype(F32)
                gathered[k, a_of(k), :, block(b_of(k))] = total.astype(gathered.dtype)
                for d in far_first:
                    ag_b(k, d, b_of(k)).start()

        def fourth(k):
            for d in near_first:
                ag_b(k, d, plus(b_of(k), N - d, N)).wait_recv()
            for d in far_first:
                ag_a(k, d, a_of(k)).start()

        def last(k):
            for d in near_first:
                ag_a(k, d, plus(a_of(k), N - d, N)).wait_recv()
            consume(k)

        def stages_of(k):
            return (first, second, third, last) if modes[k] == 3 else (first, second, third, fourth, last)

        def finish():
            for k in range(K):
                for d in range(1, N):
                    rs_a(k, d).wait_send()
                    over_b(k, d).wait_send()
                    if modes[k] == 4:
                        ag_b(k, d, b_of(k)).wait_send()
                    ag_a(k, d, a_of(k)).wait_send()

        for stage, k in stage_order(modes):
            stages_of(k)[stage](k)
        finish()

    halves = N // 2

    def token_compute(k):
        gate_loads[k].wait()
        up_loads[k].wait()
        gate = jnp.dot(scaled, gate_w[:, columns(k)], preferred_element_type=F32)
        up = jnp.dot(scaled, up_w[:, columns(k)], preferred_element_type=F32)
        gate = gate.reshape(halves, token_count // halves, C)
        up = up.reshape(halves, token_count // halves, C)
        t1_own[k, :halves] = gate
        t1_own[k, halves:] = up
        t1_src[k, :halves] = gate.astype(t1_src.dtype)
        t1_src[k, halves:] = up.astype(t1_src.dtype)

    for k in range(K):
        token_compute(k)
    pl.semaphore_wait(barrier, len(greeted))

    def token_use(k):
        gate = t_whole[k, :halves].reshape(token_count, C).astype(F32)
        up = t_whole[k, halves:].reshape(token_count, C).astype(F32)
        sigmoid = 1.0 / (1.0 + jnp.exp(-gate))
        act[:, columns(k)] = gate * sigmoid
        slope[:, columns(k)] = sigmoid * (1.0 + gate * (1.0 - sigmoid)) * up

    row_stages(
        2, lambda k: None, lambda k: t1_own[k, a_of(k)], TOKEN_MODES,
        t1_src, t1_dst, t2_src, t2_dst, t_whole, token_use,
    )
    down_load.wait()

    def by_token(values, factor):
        return (values.reshape(probe_count, token_count, C) * factor[None]).reshape(M, C)

    def send_joined(k, value):
        blocks = value.reshape(N, R, C)
        joined[k] = blocks
        p1_src[k] = blocks.astype(BF16)

    def hidden_part(k):
        lhs = pushed[...].reshape(M, width)
        gate_tan = jnp.dot(lhs, gate_w[:, columns(k)], preferred_element_type=F32)
        up_tan = jnp.dot(lhs, up_w[:, columns(k)], preferred_element_type=F32)
        send_joined(k, by_token(gate_tan, slope[:, columns(k)]) + by_token(up_tan, act[:, columns(k)]))

    def add_to_acc(k, value):
        value = value.reshape(2, half, width)
        acc[...] = value if k == 0 else acc[...] + value

    def hidden_use(k):
        lhs = whole[k].reshape(M, C)
        add_to_acc(k, jnp.dot(lhs, down_w[columns(k), :], preferred_element_type=F32))

    def back_part(k):
        lhs = tangent[...].reshape(M, width)
        send_joined(k, lax.dot_general(lhs, down_w[columns(k), :], NT, preferred_element_type=F32))

    def back_use(k):
        piece = whole[k].reshape(M, C).astype(F32)
        gate_pull = by_token(piece, slope[:, columns(k)]).astype(BF16)
        up_pull = by_token(piece, act[:, columns(k)]).astype(BF16)
        value = lax.dot_general(gate_pull, gate_w[:, columns(k)], NT, preferred_element_type=F32)
        value += lax.dot_general(up_pull, up_w[:, columns(k)], NT, preferred_element_type=F32)
        add_to_acc(k, value)

    def col_half(phase):
        swap = remote(acc.at[other], pair_in, pair_ss.at[0], pair_rs.at[0], partner)
        swap.start()
        total = acc[c]
        swap.wait_recv()
        total += pair_in[...]
        z_src[...] = total.astype(z_src.dtype)
        copies = [
            remote(z_src, z_dst.at[phase, d - 1], z_ss.at[phase, d - 1], z_rs.at[phase, d - 1], z_peer(d))
            for d in range(1, NZ)
        ]
        for d in sorted(range(1, NZ), key=lambda d: -min(d, NZ - d)):
            copies[d - 1].start()
        acc[c] = total
        swap.wait_send()
        for d in sorted(range(1, NZ), key=lambda d: min(d, NZ - d)):
            copies[d - 1].wait_recv()
        total = acc[c]
        for d in range(1, NZ):
            total += z_dst[phase, d - 1].astype(F32)
        for cp in copies:
            cp.wait_send()
        return total

    def share(buffer, which):
        mine, theirs = buffer.at[c], buffer.at[other]
        send, recv = pair_ss.at[which], pair_rs.at[which]
        remote(mine, mine, send, recv, partner).start()
        remote(theirs, theirs, send, recv, partner).wait_recv()
        remote(mine, mine, send, recv, partner).wait_send()

    def folded(values):
        rows, lanes = values.shape
        total = None
        for r in range(0, rows, 8):
            for l in range(0, lanes, 128):
                piece = values[r : r + 8, l : l + 128]
                total = piece if total is None else total + piece
        return jnp.sum(total, axis=0, keepdims=True)

    def square_copies():
        return [
            remote(sq, sq_in.at[slot], sq_ss.at[slot], sq_rs.at[slot], row_peer(dx, dy))
            for slot, (dx, dy) in enumerate(row_offsets)
        ]

    def send_squares():
        for p in range(probe_count):
            i, j = divmod(p, half_probes)
            values = grown_all[i, j * token_count : (j + 1) * token_count]
            sq[p : p + 1] = folded(values * values)
        for cp in square_copies():
            cp.start()

    def levels():
        total = sq[...]
        copies = square_copies()
        for cp in copies:
            cp.wait_recv()
        for slot in range(len(copies)):
            total += sq_in[slot]
        for cp in copies:
            cp.wait_send()
        return jnp.sum(total, axis=1, keepdims=True) / entries

    def sweep(it, carry):
        row_stages(
            0, hidden_part, lambda k: joined[k, a_of(k)], MODES, p1_src, p1_dst, p2_src, p2_dst.at[0], whole, hidden_use,
        )
        total = col_half(0)

        @pl.when(it > 0)
        def _():
            factor = lax.rsqrt(levels() + EPSILON)
            for p in range(probe_count):
                scale[p] = jnp.broadcast_to(factor[p : p + 1], scale.shape[1:])

        parts = [
            total[i * token_count : (i + 1) * token_count] * scale[c * half_probes + i, 0:1, 0:1]
            for i in range(half_probes)
        ]
        tangent[c] = jnp.concatenate(parts, axis=0).astype(BF16)
        share(tangent, 1)

        row_stages(
            1, back_part, lambda k: joined[k, a_of(k)], MODES, p1_src, p1_dst, p2_src, p2_dst.at[1], whole, back_use,
        )
        grown_all[c] = col_half(1) * gain
        share(grown_all, 2)
        send_squares()
        pushed[...] = (grown_all[...] * gain[None]).astype(BF16)
        return carry

    sq[...] = jnp.zeros_like(sq)
    lax.fori_loop(0, ITERS, sweep, 0)

    level = levels()
    root = jnp.sqrt(level)
    factor = lax.rsqrt(level + EPSILON)
    lane = lax.broadcasted_iota(jnp.int32, (1, probe_count), 1)
    stretch = jnp.zeros((1, probe_count), F32)
    for p in range(probe_count):
        stretch = jnp.where(lane == p, root[p : p + 1], stretch)
        i, j = divmod(p, half_probes)
        basis_ref[p] = grown_all[i, j * token_count : (j + 1) * token_count] * factor[p : p + 1]
    stretch_ref[...] = stretch


def solution(mesh, chunk=CHUNK, shape=(4, 4, 4, 2)):
    N, _, NZ, _ = shape
    torus = Mesh(mesh.devices.reshape(shape), ("x", "y", "z", "c"))
    row, col = ("x", "y"), ("z", "c")

    def local(tokens, gain, gate_weight, up_weight, down_weight, probes):
        probe_count, token_count, width = probes.shape
        hidden = gate_weight.shape[1]
        M = probe_count * token_count
        K, C = hidden // chunk, chunk
        R = M // N
        TR = 2 * token_count // N
        T1, T2, TG = TOKEN_TYPES
        entries = token_count * width * N * N
        cfg = (N, NZ, K, C, probe_count, token_count, entries)
        vm = pltpu.VMEM
        dma = pltpu.SemaphoreType.DMA
        basis, stretch = pl.pallas_call(
            functools.partial(kernel, cfg),
            out_shape=(
                jax.ShapeDtypeStruct(probes.shape, F32),
                jax.ShapeDtypeStruct((1, probe_count), F32),
            ),
            in_specs=[
                pl.BlockSpec(memory_space=pltpu.VMEM),
                pl.BlockSpec(memory_space=pltpu.VMEM),
                pl.BlockSpec(memory_space=pl.ANY),
                pl.BlockSpec(memory_space=pl.ANY),
                pl.BlockSpec(memory_space=pl.ANY),
                pl.BlockSpec(memory_space=pltpu.VMEM),
            ],
            out_specs=(
                pl.BlockSpec(memory_space=pltpu.VMEM),
                pl.BlockSpec(memory_space=pltpu.VMEM),
            ),
            scratch_shapes=[
                vm((width, hidden), BF16), vm((width, hidden), BF16), vm((hidden, width), BF16),
                vm((token_count, hidden), F32), vm((token_count, hidden), F32),
                vm((2, M // 2, width), BF16), vm((2, M // 2, width), BF16), vm((2, M // 2, width), F32),
                vm((2, M // 2, width), F32),
                vm((K, N, R, C), F32), vm((K, N, R, C), BF16), vm((K, N - 1, R, C), BF16),
                vm((K, R, C), BF16), vm((2, K, N - 1, R, C), BF16), vm((K, N, R, C), BF16),
                vm((K, N, TR, C), F32), vm((K, N, TR, C), T1), vm((K, N - 1, TR, C), T1),
                vm((K, TR, C), T2), vm((K, N - 1, TR, C), T2), vm((K, N, TR, C), TG),
                vm((M // 2, width), F32), vm((M // 2, width), BF16), vm((2, NZ - 1, M // 2, width), BF16),
                vm((8, 128), F32), vm((N * N - 1, 8, 128), F32),
                vm((probe_count, 8, 128), F32),
                dma((K,)), dma((K,)), dma((1,)),
                dma((K, N - 1)), dma((K, N - 1)), dma((3, K, N - 1)), dma((3, K, N - 1)),
                *[dma((K, N - 1)) for _ in range(4)],
                dma((3,)), dma((3,)),
                dma((2, NZ - 1)), dma((2, NZ - 1)),
                dma((N * N - 1,)), dma((N * N - 1,)),
            ],
            compiler_params=pltpu.CompilerParams(collective_id=0, has_side_effects=True),
        )(tokens, gain.reshape(1, width), gate_weight, up_weight, down_weight, probes)
        return basis, stretch.reshape(probe_count)

    return jax.shard_map(
        local,
        mesh=torus,
        in_specs=(P(None, row), P(row), P(row, col), P(row, col), P(col, row), P(None, None, row)),
        out_specs=(P(None, None, row), P()),
        check_vma=False,
    )
```

```python
import functools

import jax
import jax.numpy as jnp
from jax import lax
from jax.experimental import pallas as pl
from jax.experimental.pallas import tpu as pltpu
from jax.sharding import Mesh
from jax.sharding import PartitionSpec as P

ITERS = 3
EPSILON = 1e-06
MESH = pl.DeviceIdType.MESH
F32 = jnp.float32
BF16 = jnp.bfloat16
NT = (((1,), (1,)), ((), ()))
CHUNK = 512
MODES = (3, 3, 3, 3, 3, 3, 3)
TOKEN_MODES = (3, 3, 3, 3, 3, 3, 3)
TOKEN_TYPES = (BF16, F32, F32)
HOP = 3.0
STEP = 0.5


def stage_order(modes):
    events = []
    for k, mode in enumerate(modes):
        events.append((0.3 * k, 0, k))
        for stage in range(1, mode + 1):
            events.append((1.0 + STEP * (k + 1) + HOP * stage, stage, k))
    return [(stage, k) for _, stage, k in sorted(events)]


def kernel(
    cfg,
    tokens_hbm, gain_hbm, gate_hbm, up_hbm, down_hbm, probes_hbm,
    grown_hbm, level_ref,
    tokens_ref, gain_ref, probes_ref, gate_w, up_w, down_w,
    slope, act, pushed, tangent, grown_all, acc,
    joined, p1_src, p1_dst, p2_src, p2_dst, whole,
    t1_own, t1_src, t1_dst, t2_src, t2_dst, t_whole,
    pair_in, z_src, z_dst, sq, sq_in, scale,
    small_sem, gate_sem, up_sem, down_sem, p1_ss, p1_rs, p2_ss, p2_rs, g1_ss, g1_rs, g2_ss, g2_rs,
    pair_ss, pair_rs, z_ss, z_rs, sq_ss, sq_rs,
):
    N, NZ, K, C, probe_count, token_count, entries = cfg
    M = probe_count * token_count
    R = M // N
    W = C // N
    half = M // 2
    half_probes = probe_count // 2
    width = gain_ref.shape[1]
    x, y, z, c = (lax.axis_index(name) for name in ("x", "y", "z", "c"))
    other = 1 - c
    def around(v, n):
        return [v] + [lax.rem(v + d, n) for d in range(1, n)]

    xs, ys, zs = around(x, N), around(y, N), around(z, NZ)

    def device(i, j, k, core):
        return (i, j, k, core)

    a_at = (
        [xs[d] * other + ys[d] * c for d in range(N)],
        [ys[d] * other + xs[d] * c for d in range(N)],
    )
    a_devices = (
        [device(xs[d] * other + x * c, y * other + ys[d] * c, z, c) for d in range(N)],
        [device(xs[d] * c + x * other, y * c + ys[d] * other, z, c) for d in range(N)],
    )

    def a_of(k, d=0):
        return a_at[k % 2][d]

    def b_of(k, d=0):
        return a_at[1 - k % 2][d]

    def a_peer(k, d):
        return a_devices[k % 2][d]

    def b_peer(k, d):
        return a_devices[1 - k % 2][d]

    def row_peer(dx, dy):
        return device(xs[dx], ys[dy], z, c)

    z_peers = [device(x, y, zs[d], c) for d in range(NZ)]
    partner = device(x, y, z, other)
    row_offsets = [(dx, dy) for dx in range(N) for dy in range(N) if dx or dy]

    def columns(k):
        return slice(k * C, (k + 1) * C)

    def remote(src, dst, send, recv, target):
        return pltpu.make_async_remote_copy(
            src_ref=src, dst_ref=dst, send_sem=send, recv_sem=recv,
            device_id=target, device_id_type=MESH,
        )

    def wait_for(ref, sem):
        pltpu.make_async_copy(ref, ref, sem).wait()

    gate_loads = [
        pltpu.make_async_copy(gate_hbm.at[:, columns(k)], gate_w.at[:, columns(k)], gate_sem.at[k])
        for k in range(K)
    ]
    up_loads = [
        pltpu.make_async_copy(up_hbm.at[:, columns(k)], up_w.at[:, columns(k)], up_sem.at[k])
        for k in range(K)
    ]
    down_load = pltpu.make_async_copy(down_hbm, down_w, down_sem.at[0])
    tokens_load = pltpu.make_async_copy(tokens_hbm, tokens_ref, small_sem.at[0])
    gain_load = pltpu.make_async_copy(gain_hbm, gain_ref, small_sem.at[1])
    probes_load = pltpu.make_async_copy(probes_hbm, probes_ref, small_sem.at[2])
    tokens_load.start()
    gain_load.start()
    for k in range(K):
        gate_loads[k].start()
        up_loads[k].start()
    probes_load.start()
    down_load.start()

    barrier = pltpu.get_barrier_semaphore()
    greeted = [row_peer(dx, dy) for dx, dy in row_offsets]
    greeted += [z_peers[d] for d in range(1, NZ)] + [partner]
    for target in greeted:
        pl.semaphore_signal(barrier, inc=1, device_id=target, device_id_type=MESH)

    tokens_load.wait()
    gain_load.wait()
    gain = gain_ref[...]
    scaled = (tokens_ref[...].astype(F32) * gain).astype(BF16)

    far_first = sorted(range(1, N), key=lambda d: -min(d, N - d))
    near_first = far_first[::-1]

    def row_stages(phase, part, modes, src, dst, src2, dst2, gathered, consume, after_first=None):
        def block(j):
            return pl.ds(pl.multiple_of(j * W, W), W)

        def rs_a(k, d):
            return remote(src.at[k, a_of(k, d)], dst.at[k, d - 1], p1_ss.at[0], p1_rs.at[k], a_peer(k, d))

        def over_b(k, d):
            if modes[k] == 3:
                sent, taken = src2.at[k], dst2.at[k, d - 1]
            else:
                sent, taken = src2.at[k, :, block(b_of(k, d))], dst2.at[k, d - 1, :, 0:W]
            return remote(sent, taken, p2_ss.at[0], p2_rs.at[phase, k], b_peer(k, d))

        def ag_b(k, d):
            piece = gathered.at[k, a_of(k), :, block(b_of(k))]
            return remote(piece, piece, g1_ss.at[0], g1_rs.at[k], b_peer(k, d))

        def ag_a(k, d):
            piece = gathered.at[k, a_of(k)]
            return remote(piece, piece, g2_ss.at[0], g2_rs.at[k], a_peer(k, d))

        def first(k):
            part(k)
            for d in far_first:
                rs_a(k, d).start()

        kept = joined if src is p1_src else t1_own

        def second(k):
            wait_for(dst.at[k], p1_rs.at[k])
            total = kept[k, a_of(k)]
            for d in near_first:
                total += dst[k, d - 1].astype(F32)
            src2[k] = total.astype(src2.dtype)
            for d in far_first:
                over_b(k, d).start()
            kept[k, a_of(k)] = total

        def third(k):
            if modes[k] == 3:
                wait_for(dst2.at[k], p2_rs.at[phase, k])
                total = kept[k, a_of(k)]
                for d in near_first:
                    total += dst2[k, d - 1].astype(F32)
                gathered[k, a_of(k)] = total.astype(gathered.dtype)
                for d in far_first:
                    ag_a(k, d).start()
            else:
                wait_for(dst2.at[k, :, :, 0:W], p2_rs.at[phase, k])
                total = kept[k, a_of(k), :, block(b_of(k))]
                for d in near_first:
                    total += dst2[k, d - 1, :, 0:W].astype(F32)
                gathered[k, a_of(k), :, block(b_of(k))] = total.astype(gathered.dtype)
                for d in far_first:
                    ag_b(k, d).start()

        def fourth(k):
            wait_for(gathered.at[k, a_of(k), :, 0 : (N - 1) * W], g1_rs.at[k])
            for d in far_first:
                ag_a(k, d).start()

        def last(k):
            wait_for(gathered.at[k, 0 : N - 1], g2_rs.at[k])
            consume(k)

        def stages_of(k):
            return (first, second, third, last) if modes[k] == 3 else (first, second, third, fourth, last)

        wide = [k for k in range(K) if modes[k] == 3]
        narrow = [k for k in range(K) if modes[k] == 4]

        def finish():
            wait_for(dst, p1_ss.at[0])
            if narrow:
                wait_for(dst2.at[0 : len(narrow), :, :, 0:W], p2_ss.at[0])
                wait_for(gathered.at[0 : len(narrow), 0 : N - 1, :, 0:W], g1_ss.at[0])
            if wide:
                wait_for(dst2.at[0 : len(wide)], p2_ss.at[0])
            wait_for(gathered.at[:, 0 : N - 1], g2_ss.at[0])

        hook = after_first
        for stage, k in stage_order(modes):
            if stage and hook is not None:
                hook()
                hook = None
            stages_of(k)[stage](k)
        return finish

    halves = N // 2

    def token_compute(k):
        gate_loads[k].wait()
        up_loads[k].wait()
        gate = jnp.dot(scaled, gate_w[:, columns(k)], preferred_element_type=F32)
        up = jnp.dot(scaled, up_w[:, columns(k)], preferred_element_type=F32)
        gate = gate.reshape(halves, token_count // halves, C)
        up = up.reshape(halves, token_count // halves, C)
        t1_own[k, :halves] = gate
        t1_own[k, halves:] = up
        t1_src[k, :halves] = gate.astype(t1_src.dtype)
        t1_src[k, halves:] = up.astype(t1_src.dtype)

    for k in range(K):
        token_compute(k)
    pl.semaphore_wait(barrier, len(greeted))

    def token_use(k):
        gate = t_whole[k, :halves].reshape(token_count, C).astype(F32)
        up = t_whole[k, halves:].reshape(token_count, C).astype(F32)
        sigmoid = 1.0 / (1.0 + jnp.exp(-gate))
        act[:, columns(k)] = gate * sigmoid
        slope[:, columns(k)] = sigmoid * (1.0 + gate * (1.0 - sigmoid)) * up

    def start_probes():
        probes_load.wait()
        pushed[...] = (probes_ref[...] * gain[None]).astype(BF16).reshape(2, half, width)
        scale[...] = jnp.ones_like(scale)
        down_load.wait()

    row_stages(
        2, lambda k: None, TOKEN_MODES,
        t1_src, t1_dst, t2_src, t2_dst, t_whole, token_use, start_probes,
    )()

    def by_token(values, factor):
        return (values.reshape(probe_count, token_count, C) * factor[None]).reshape(M, C)

    def send_joined(k, value):
        blocks = value.reshape(N, R, C)
        joined[k] = blocks
        p1_src[k] = blocks.astype(BF16)

    def hidden_part(k):
        lhs = pushed[...].reshape(M, width)
        gate_tan = jnp.dot(lhs, gate_w[:, columns(k)], preferred_element_type=F32)
        up_tan = jnp.dot(lhs, up_w[:, columns(k)], preferred_element_type=F32)
        send_joined(k, by_token(gate_tan, slope[:, columns(k)]) + by_token(up_tan, act[:, columns(k)]))

    def add_to_acc(k, value):
        value = value.reshape(2, half, width)
        acc[...] = value if k == 0 else acc[...] + value

    def hidden_use(k):
        lhs = whole[k].reshape(M, C)
        add_to_acc(k, jnp.dot(lhs, down_w[columns(k), :], preferred_element_type=F32))

    def back_part(k):
        lhs = tangent[...].reshape(M, width)
        send_joined(k, lax.dot_general(lhs, down_w[columns(k), :], NT, preferred_element_type=F32))

    def back_use(k):
        piece = whole[k].reshape(M, C).astype(F32)
        gate_pull = by_token(piece, slope[:, columns(k)]).astype(BF16)
        up_pull = by_token(piece, act[:, columns(k)]).astype(BF16)
        value = lax.dot_general(gate_pull, gate_w[:, columns(k)], NT, preferred_element_type=F32)
        value += lax.dot_general(up_pull, up_w[:, columns(k)], NT, preferred_element_type=F32)
        add_to_acc(k, value)

    def col_half(phase, finish_row):
        swap = remote(acc.at[other], pair_in, pair_ss.at[0], pair_rs.at[0], partner)
        swap.start()
        total = acc[c]
        swap.wait_recv()
        total += pair_in[...]
        z_src[...] = total.astype(z_src.dtype)
        copies = [
            remote(z_src, z_dst.at[phase, d - 1], z_ss.at[0], z_rs.at[phase], z_peers[d])
            for d in range(1, NZ)
        ]
        for d in sorted(range(1, NZ), key=lambda d: -min(d, NZ - d)):
            copies[d - 1].start()
        acc[c] = total
        swap.wait_send()
        finish_row()
        wait_for(z_dst.at[phase], z_rs.at[phase])
        total = acc[c]
        for d in range(1, NZ):
            total += z_dst[phase, d - 1].astype(F32)
        wait_for(z_dst.at[phase], z_ss.at[0])
        return total

    def share(buffer, which):
        mine, theirs = buffer.at[c], buffer.at[other]
        send, recv = pair_ss.at[which], pair_rs.at[which]
        remote(mine, mine, send, recv, partner).start()
        remote(theirs, theirs, send, recv, partner).wait_recv()
        remote(mine, mine, send, recv, partner).wait_send()

    def folded(values):
        rows, lanes = values.shape
        total = None
        for r in range(0, rows, 8):
            for l in range(0, lanes, 128):
                piece = values[r : r + 8, l : l + 128]
                total = piece if total is None else total + piece
        return jnp.sum(total, axis=0, keepdims=True)

    def square_copies():
        return [
            remote(sq, sq_in.at[slot], sq_ss.at[0], sq_rs.at[0], row_peer(dx, dy))
            for slot, (dx, dy) in enumerate(row_offsets)
        ]

    def send_squares():
        for p in range(probe_count):
            i, j = divmod(p, half_probes)
            values = grown_all[i, j * token_count : (j + 1) * token_count]
            sq[p : p + 1] = folded(values * values)
        for cp in square_copies():
            cp.start()

    def levels():
        total = sq[...]
        wait_for(sq_in, sq_rs.at[0])
        for slot in range(len(row_offsets)):
            total += sq_in[slot]
        wait_for(sq_in, sq_ss.at[0])
        return jnp.sum(total, axis=1, keepdims=True) / entries

    def sweep(it, carry):
        def squares():
            @pl.when(it > 0)
            def _():
                send_squares()

        finish = row_stages(
            0, hidden_part, MODES,
            p1_src, p1_dst, p2_src, p2_dst.at[0], whole, hidden_use, squares,
        )
        total = col_half(0, finish)

        @pl.when(it > 0)
        def _():
            factor = lax.rsqrt(levels() + EPSILON)
            for p in range(probe_count):
                scale[p] = jnp.broadcast_to(factor[p : p + 1], scale.shape[1:])

        parts = [
            total[i * token_count : (i + 1) * token_count] * scale[c * half_probes + i, 0:1, 0:1]
            for i in range(half_probes)
        ]
        tangent[c] = jnp.concatenate(parts, axis=0).astype(BF16)
        share(tangent, 1)

        finish = row_stages(
            1, back_part, MODES,
            p1_src, p1_dst, p2_src, p2_dst.at[1], whole, back_use,
        )
        grown_all[c] = col_half(1, finish) * gain
        share(grown_all, 2)
        pushed[...] = (grown_all[...] * gain[None]).astype(BF16)
        return carry

    sq[...] = jnp.zeros_like(sq)
    lax.fori_loop(0, ITERS, sweep, 0)

    send_squares()
    out = pltpu.make_async_copy(grown_all, grown_hbm, small_sem.at[3])
    out.start()
    level_ref[...] = jnp.broadcast_to(levels(), level_ref.shape)
    out.wait()


def finish_kernel(grown_ref, level_ref, basis_ref, stretch_ref):
    probe_count = basis_ref.shape[0]
    level = level_ref[...]
    root = jnp.sqrt(level)
    factor = lax.rsqrt(level + EPSILON)
    lane = lax.broadcasted_iota(jnp.int32, (1, probe_count), 1)
    stretch = jnp.zeros((1, probe_count), F32)
    for p in range(probe_count):
        stretch = jnp.where(lane == p, root[p : p + 1, 0:1], stretch)
        basis_ref[p] = grown_ref[p] * factor[p : p + 1, 0:1]
    stretch_ref[...] = stretch


def solution(mesh, chunk=CHUNK, shape=(4, 4, 4, 2)):
    N, _, NZ, _ = shape
    torus = Mesh(mesh.devices.reshape(shape), ("x", "y", "z", "c"))
    row, col = ("x", "y"), ("z", "c")

    def local(tokens, gain, gate_weight, up_weight, down_weight, probes):
        probe_count, token_count, width = probes.shape
        hidden = gate_weight.shape[1]
        M = probe_count * token_count
        K, C = hidden // chunk, chunk
        R = M // N
        TR = 2 * token_count // N
        T1, T2, TG = TOKEN_TYPES
        entries = token_count * width * N * N
        cfg = (N, NZ, K, C, probe_count, token_count, entries)
        vm = pltpu.VMEM
        dma = pltpu.SemaphoreType.DMA
        grown, level = pl.pallas_call(
            functools.partial(kernel, cfg),
            out_shape=(
                jax.ShapeDtypeStruct((2, M // 2, width), F32),
                jax.ShapeDtypeStruct((8, 128), F32),
            ),
            in_specs=[pl.BlockSpec(memory_space=pl.ANY)] * 6,
            out_specs=(
                pl.BlockSpec(memory_space=pl.ANY),
                pl.BlockSpec(memory_space=pltpu.VMEM),
            ),
            scratch_shapes=[
                vm((token_count, width), BF16), vm((1, width), F32), vm(probes.shape, F32),
                vm((width, hidden), BF16), vm((width, hidden), BF16), vm((hidden, width), BF16),
                vm((token_count, hidden), F32), vm((token_count, hidden), F32),
                vm((2, M // 2, width), BF16), vm((2, M // 2, width), BF16), vm((2, M // 2, width), F32),
                vm((2, M // 2, width), F32),
                vm((K, N, R, C), F32), vm((K, N, R, C), BF16), vm((K, N - 1, R, C), BF16),
                vm((K, R, C), BF16), vm((2, K, N - 1, R, C), BF16), vm((K, N, R, C), BF16),
                vm((K, N, TR, C), F32), vm((K, N, TR, C), T1), vm((K, N - 1, TR, C), T1),
                vm((K, TR, C), T2), vm((K, N - 1, TR, C), T2), vm((K, N, TR, C), TG),
                vm((M // 2, width), F32), vm((M // 2, width), BF16), vm((2, NZ - 1, M // 2, width), BF16),
                vm((8, 128), F32), vm((N * N - 1, 8, 128), F32),
                vm((probe_count, 8, 128), F32),
                dma((4,)), dma((K,)), dma((K,)), dma((1,)),
                dma((1,)), dma((K,)), dma((1,)), dma((3, K)), dma((1,)), dma((K,)), dma((1,)), dma((K,)),
                dma((3,)), dma((3,)),
                dma((1,)), dma((2,)),
                dma((1,)), dma((1,)),
            ],
            compiler_params=pltpu.CompilerParams(collective_id=0, has_side_effects=True),
        )(tokens, gain.reshape(1, width), gate_weight, up_weight, down_weight, probes)
        basis, stretch = pl.pallas_call(
            finish_kernel,
            out_shape=(
                jax.ShapeDtypeStruct(probes.shape, F32),
                jax.ShapeDtypeStruct((1, probe_count), F32),
            ),
            in_specs=[pl.BlockSpec(memory_space=pltpu.VMEM)] * 2,
            out_specs=(
                pl.BlockSpec(memory_space=pltpu.VMEM),
                pl.BlockSpec(memory_space=pltpu.VMEM),
            ),
        )(grown.reshape(probes.shape), level)
        return basis, stretch.reshape(probe_count)

    return jax.shard_map(
        local,
        mesh=torus,
        in_specs=(P(None, row), P(row), P(row, col), P(row, col), P(col, row), P(None, None, row)),
        out_specs=(P(None, None, row), P()),
        check_vma=False,
    )
```

```python
import functools

import jax
import jax.numpy as jnp
from jax import lax
from jax.experimental import pallas as pl
from jax.experimental.pallas import tpu as pltpu
from jax.sharding import Mesh
from jax.sharding import PartitionSpec as P

ITERS = 3
EPSILON = 1e-06
MESH = pl.DeviceIdType.MESH
F32 = jnp.float32
BF16 = jnp.bfloat16
NT = (((1,), (1,)), ((), ()))
CHUNK = 512
MODES = (3, 3, 3, 3, 3, 3, 3)
TOKEN_MODES = (3, 3, 3, 3, 3, 3, 3)
TOKEN_TYPES = (BF16, BF16, F32)
HOP = 3.0
STEP = 0.5


def stage_order(modes):
    events = []
    for k, mode in enumerate(modes):
        events.append((0.3 * k, 0, k))
        for stage in range(1, mode + 1):
            events.append((1.0 + STEP * (k + 1) + HOP * stage, stage, k))
    return [(stage, k) for _, stage, k in sorted(events)]


def kernel(
    cfg,
    tokens_hbm, gain_hbm, gate_hbm, up_hbm, down_hbm, probes_hbm,
    grown_hbm, level_ref,
    tokens_ref, gain_ref, probes_ref, gate_w, up_w, down_w,
    slope, act, pushed, tangent, grown_all, acc,
    joined, p1_src, p1_dst, p2_src, p2_dst, whole,
    t1_own, t1_src, t1_dst, t2_src, t2_dst, t_whole,
    pair_in, z_src, z_dst, sq, sq_in, scale,
    small_sem, gate_sem, up_sem, down_sem, p1_ss, p1_rs, p2_ss, p2_rs, g1_ss, g1_rs, g2_ss, g2_rs,
    pair_ss, pair_rs, z_ss, z_rs, sq_ss, sq_rs,
):
    N, NZ, K, C, probe_count, token_count, entries = cfg
    M = probe_count * token_count
    R = M // N
    W = C // N
    half = M // 2
    half_probes = probe_count // 2
    width = gain_ref.shape[1]
    x, y, z, c = (lax.axis_index(name) for name in ("x", "y", "z", "c"))
    other = 1 - c
    def around(v, n):
        return [v] + [lax.rem(v + d, n) for d in range(1, n)]

    xs, ys, zs = around(x, N), around(y, N), around(z, NZ)

    def device(i, j, k, core):
        return (i, j, k, core)

    a_at = (
        [xs[d] * other + ys[d] * c for d in range(N)],
        [ys[d] * other + xs[d] * c for d in range(N)],
    )
    a_devices = (
        [device(xs[d] * other + x * c, y * other + ys[d] * c, z, c) for d in range(N)],
        [device(xs[d] * c + x * other, y * c + ys[d] * other, z, c) for d in range(N)],
    )

    def a_of(k, d=0):
        return a_at[k % 2][d]

    def b_of(k, d=0):
        return a_at[1 - k % 2][d]

    def a_peer(k, d):
        return a_devices[k % 2][d]

    def b_peer(k, d):
        return a_devices[1 - k % 2][d]

    def row_peer(dx, dy):
        return device(xs[dx], ys[dy], z, c)

    z_peers = [device(x, y, zs[d], c) for d in range(NZ)]
    partner = device(x, y, z, other)
    row_offsets = [(dx, dy) for dx in range(N) for dy in range(N) if dx or dy]

    def columns(k):
        return slice(k * C, (k + 1) * C)

    def remote(src, dst, send, recv, target):
        return pltpu.make_async_remote_copy(
            src_ref=src, dst_ref=dst, send_sem=send, recv_sem=recv,
            device_id=target, device_id_type=MESH,
        )

    def wait_for(ref, sem):
        pltpu.make_async_copy(ref, ref, sem).wait()

    gate_loads = [
        pltpu.make_async_copy(gate_hbm.at[:, columns(k)], gate_w.at[:, columns(k)], gate_sem.at[k])
        for k in range(K)
    ]
    up_loads = [
        pltpu.make_async_copy(up_hbm.at[:, columns(k)], up_w.at[:, columns(k)], up_sem.at[k])
        for k in range(K)
    ]
    down_load = pltpu.make_async_copy(down_hbm, down_w, down_sem.at[0])
    tokens_load = pltpu.make_async_copy(tokens_hbm, tokens_ref, small_sem.at[0])
    gain_load = pltpu.make_async_copy(gain_hbm, gain_ref, small_sem.at[1])
    probes_load = pltpu.make_async_copy(probes_hbm, probes_ref, small_sem.at[2])
    tokens_load.start()
    gain_load.start()
    for k in range(K):
        gate_loads[k].start()
        up_loads[k].start()
    probes_load.start()
    down_load.start()

    barrier = pltpu.get_barrier_semaphore()
    greeted = [row_peer(dx, dy) for dx, dy in row_offsets]
    greeted += [z_peers[d] for d in range(1, NZ)] + [partner]
    for target in greeted:
        pl.semaphore_signal(barrier, inc=1, device_id=target, device_id_type=MESH)

    tokens_load.wait()
    gain_load.wait()
    gain = gain_ref[...]
    scaled = (tokens_ref[...].astype(F32) * gain).astype(BF16)

    far_first = sorted(range(1, N), key=lambda d: -min(d, N - d))
    near_first = far_first[::-1]

    def row_stages(phase, part, modes, src, dst, src2, dst2, gathered, consume, after_first=None):
        def block(j):
            return pl.ds(pl.multiple_of(j * W, W), W)

        def rs_a(k, d):
            return remote(src.at[k, a_of(k, d)], dst.at[k, d - 1], p1_ss.at[0], p1_rs.at[k], a_peer(k, d))

        def over_b(k, d):
            if modes[k] == 3:
                sent, taken = src2.at[k], dst2.at[k, d - 1]
            else:
                sent, taken = src2.at[k, :, block(b_of(k, d))], dst2.at[k, d - 1, :, 0:W]
            return remote(sent, taken, p2_ss.at[0], p2_rs.at[phase, k], b_peer(k, d))

        def ag_b(k, d):
            piece = gathered.at[k, a_of(k), :, block(b_of(k))]
            return remote(piece, piece, g1_ss.at[0], g1_rs.at[k], b_peer(k, d))

        def ag_a(k, d):
            piece = gathered.at[k, a_of(k)]
            return remote(piece, piece, g2_ss.at[0], g2_rs.at[k], a_peer(k, d))

        def first(k):
            part(k)
            for d in far_first:
                rs_a(k, d).start()

        kept = joined if src is p1_src else t1_own

        def second(k):
            wait_for(dst.at[k], p1_rs.at[k])
            total = kept[k, a_of(k)]
            for d in near_first:
                total += dst[k, d - 1].astype(F32)
            src2[k] = total.astype(src2.dtype)
            for d in far_first:
                over_b(k, d).start()
            kept[k, a_of(k)] = total

        def third(k):
            if modes[k] == 3:
                wait_for(dst2.at[k], p2_rs.at[phase, k])
                total = kept[k, a_of(k)]
                for d in near_first:
                    total += dst2[k, d - 1].astype(F32)
                gathered[k, a_of(k)] = total.astype(gathered.dtype)
                for d in far_first:
                    ag_a(k, d).start()
            else:
                wait_for(dst2.at[k, :, :, 0:W], p2_rs.at[phase, k])
                total = kept[k, a_of(k), :, block(b_of(k))]
                for d in near_first:
                    total += dst2[k, d - 1, :, 0:W].astype(F32)
                gathered[k, a_of(k), :, block(b_of(k))] = total.astype(gathered.dtype)
                for d in far_first:
                    ag_b(k, d).start()

        def fourth(k):
            wait_for(gathered.at[k, a_of(k), :, 0 : (N - 1) * W], g1_rs.at[k])
            for d in far_first:
                ag_a(k, d).start()

        def last(k):
            wait_for(gathered.at[k, 0 : N - 1], g2_rs.at[k])
            consume(k)

        def stages_of(k):
            return (first, second, third, last) if modes[k] == 3 else (first, second, third, fourth, last)

        wide = [k for k in range(K) if modes[k] == 3]
        narrow = [k for k in range(K) if modes[k] == 4]

        def finish():
            wait_for(dst, p1_ss.at[0])
            if narrow:
                wait_for(dst2.at[0 : len(narrow), :, :, 0:W], p2_ss.at[0])
                wait_for(gathered.at[0 : len(narrow), 0 : N - 1, :, 0:W], g1_ss.at[0])
            if wide:
                wait_for(dst2.at[0 : len(wide)], p2_ss.at[0])
            wait_for(gathered.at[:, 0 : N - 1], g2_ss.at[0])

        hook = after_first
        for stage, k in stage_order(modes):
            if stage and hook is not None:
                hook()
                hook = None
            stages_of(k)[stage](k)
        return finish

    halves = N // 2

    def token_compute(k):
        gate_loads[k].wait()
        up_loads[k].wait()
        gate = jnp.dot(scaled, gate_w[:, columns(k)], preferred_element_type=F32)
        up = jnp.dot(scaled, up_w[:, columns(k)], preferred_element_type=F32)
        gate = gate.reshape(halves, token_count // halves, C)
        up = up.reshape(halves, token_count // halves, C)
        t1_own[k, :halves] = gate
        t1_own[k, halves:] = up
        t1_src[k, :halves] = gate.astype(t1_src.dtype)
        t1_src[k, halves:] = up.astype(t1_src.dtype)

    for k in range(K):
        token_compute(k)
    pl.semaphore_wait(barrier, len(greeted))

    def token_use(k):
        gate = t_whole[k, :halves].reshape(token_count, C).astype(F32)
        up = t_whole[k, halves:].reshape(token_count, C).astype(F32)
        sigmoid = 1.0 / (1.0 + jnp.exp(-gate))
        act[:, columns(k)] = gate * sigmoid
        slope[:, columns(k)] = sigmoid * (1.0 + gate * (1.0 - sigmoid)) * up

    def start_probes():
        probes_load.wait()
        pushed[...] = (probes_ref[...] * gain[None]).astype(BF16).reshape(2, half, width)
        scale[...] = jnp.ones_like(scale)
        down_load.wait()

    row_stages(
        2, lambda k: None, TOKEN_MODES,
        t1_src, t1_dst, t2_src, t2_dst, t_whole, token_use, start_probes,
    )()

    def by_token(values, factor):
        return (values.reshape(probe_count, token_count, C) * factor[None]).reshape(M, C)

    def send_joined(k, value):
        blocks = value.reshape(N, R, C)
        joined[k] = blocks
        p1_src[k] = blocks.astype(BF16)

    def hidden_part(k):
        lhs = pushed[...].reshape(M, width)
        gate_tan = jnp.dot(lhs, gate_w[:, columns(k)], preferred_element_type=F32)
        up_tan = jnp.dot(lhs, up_w[:, columns(k)], preferred_element_type=F32)
        send_joined(k, by_token(gate_tan, slope[:, columns(k)]) + by_token(up_tan, act[:, columns(k)]))

    def add_to_acc(k, value):
        value = value.reshape(2, half, width)
        acc[...] = value if k == 0 else acc[...] + value

    def hidden_use(k):
        lhs = whole[k].reshape(M, C)
        add_to_acc(k, jnp.dot(lhs, down_w[columns(k), :], preferred_element_type=F32))

    def back_part(k):
        lhs = tangent[...].reshape(M, width)
        send_joined(k, lax.dot_general(lhs, down_w[columns(k), :], NT, preferred_element_type=F32))

    def back_use(k):
        piece = whole[k].reshape(M, C).astype(F32)
        gate_pull = by_token(piece, slope[:, columns(k)]).astype(BF16)
        up_pull = by_token(piece, act[:, columns(k)]).astype(BF16)
        value = lax.dot_general(gate_pull, gate_w[:, columns(k)], NT, preferred_element_type=F32)
        value += lax.dot_general(up_pull, up_w[:, columns(k)], NT, preferred_element_type=F32)
        add_to_acc(k, value)

    def col_half(phase, finish_row):
        swap = remote(acc.at[other], pair_in, pair_ss.at[0], pair_rs.at[0], partner)
        swap.start()
        total = acc[c]
        swap.wait_recv()
        total += pair_in[...]
        z_src[...] = total.astype(z_src.dtype)
        copies = [
            remote(z_src, z_dst.at[phase, d - 1], z_ss.at[0], z_rs.at[phase], z_peers[d])
            for d in range(1, NZ)
        ]
        for d in sorted(range(1, NZ), key=lambda d: -min(d, NZ - d)):
            copies[d - 1].start()
        acc[c] = total
        swap.wait_send()
        finish_row()
        wait_for(z_dst.at[phase], z_rs.at[phase])
        total = acc[c]
        for d in range(1, NZ):
            total += z_dst[phase, d - 1].astype(F32)
        wait_for(z_dst.at[phase], z_ss.at[0])
        return total

    def share(buffer, which):
        mine, theirs = buffer.at[c], buffer.at[other]
        send, recv = pair_ss.at[which], pair_rs.at[which]
        remote(mine, mine, send, recv, partner).start()
        remote(theirs, theirs, send, recv, partner).wait_recv()
        remote(mine, mine, send, recv, partner).wait_send()

    def folded(values):
        rows, lanes = values.shape
        total = None
        for r in range(0, rows, 8):
            for l in range(0, lanes, 128):
                piece = values[r : r + 8, l : l + 128]
                total = piece if total is None else total + piece
        return jnp.sum(total, axis=0, keepdims=True)

    def square_copies():
        return [
            remote(sq, sq_in.at[slot], sq_ss.at[0], sq_rs.at[0], row_peer(dx, dy))
            for slot, (dx, dy) in enumerate(row_offsets)
        ]

    def send_squares():
        for p in range(probe_count):
            i, j = divmod(p, half_probes)
            values = grown_all[i, j * token_count : (j + 1) * token_count]
            sq[p : p + 1] = folded(values * values)
        for cp in square_copies():
            cp.start()

    def levels():
        total = sq[...]
        wait_for(sq_in, sq_rs.at[0])
        for slot in range(len(row_offsets)):
            total += sq_in[slot]
        wait_for(sq_in, sq_ss.at[0])
        return jnp.sum(total, axis=1, keepdims=True) / entries

    def sweep(it, carry):
        def squares():
            @pl.when(it > 0)
            def _():
                send_squares()

        finish = row_stages(
            0, hidden_part, MODES,
            p1_src, p1_dst, p2_src, p2_dst.at[0], whole, hidden_use, squares,
        )
        total = col_half(0, finish)

        @pl.when(it > 0)
        def _():
            factor = lax.rsqrt(levels() + EPSILON)
            for p in range(probe_count):
                scale[p] = jnp.broadcast_to(factor[p : p + 1], scale.shape[1:])

        parts = [
            total[i * token_count : (i + 1) * token_count] * scale[c * half_probes + i, 0:1, 0:1]
            for i in range(half_probes)
        ]
        tangent[c] = jnp.concatenate(parts, axis=0).astype(BF16)
        share(tangent, 1)

        finish = row_stages(
            1, back_part, MODES,
            p1_src, p1_dst, p2_src, p2_dst.at[1], whole, back_use,
        )
        grown_all[c] = col_half(1, finish) * gain
        share(grown_all, 2)
        pushed[...] = (grown_all[...] * gain[None]).astype(BF16)
        return carry

    sq[...] = jnp.zeros_like(sq)
    lax.fori_loop(0, ITERS, sweep, 0)

    send_squares()
    out = pltpu.make_async_copy(grown_all, grown_hbm, small_sem.at[3])
    out.start()
    level_ref[...] = jnp.broadcast_to(levels(), level_ref.shape)
    out.wait()


def finish_kernel(grown_ref, level_ref, basis_ref, stretch_ref):
    probe_count = basis_ref.shape[0]
    level = level_ref[...]
    root = jnp.sqrt(level)
    factor = lax.rsqrt(level + EPSILON)
    lane = lax.broadcasted_iota(jnp.int32, (1, probe_count), 1)
    stretch = jnp.zeros((1, probe_count), F32)
    for p in range(probe_count):
        stretch = jnp.where(lane == p, root[p : p + 1, 0:1], stretch)
        basis_ref[p] = grown_ref[p] * factor[p : p + 1, 0:1]
    stretch_ref[...] = stretch


def solution(mesh, chunk=CHUNK, shape=(4, 4, 4, 2)):
    N, _, NZ, _ = shape
    torus = Mesh(mesh.devices.reshape(shape), ("x", "y", "z", "c"))
    row, col = ("x", "y"), ("z", "c")

    def local(tokens, gain, gate_weight, up_weight, down_weight, probes):
        probe_count, token_count, width = probes.shape
        hidden = gate_weight.shape[1]
        M = probe_count * token_count
        K, C = hidden // chunk, chunk
        R = M // N
        TR = 2 * token_count // N
        T1, T2, TG = TOKEN_TYPES
        entries = token_count * width * N * N
        cfg = (N, NZ, K, C, probe_count, token_count, entries)
        vm = pltpu.VMEM
        dma = pltpu.SemaphoreType.DMA
        grown, level = pl.pallas_call(
            functools.partial(kernel, cfg),
            out_shape=(
                jax.ShapeDtypeStruct((2, M // 2, width), F32),
                jax.ShapeDtypeStruct((8, 128), F32),
            ),
            in_specs=[pl.BlockSpec(memory_space=pl.ANY)] * 6,
            out_specs=(
                pl.BlockSpec(memory_space=pl.ANY),
                pl.BlockSpec(memory_space=pltpu.VMEM),
            ),
            scratch_shapes=[
                vm((token_count, width), BF16), vm((1, width), F32), vm(probes.shape, F32),
                vm((width, hidden), BF16), vm((width, hidden), BF16), vm((hidden, width), BF16),
                vm((token_count, hidden), F32), vm((token_count, hidden), F32),
                vm((2, M // 2, width), BF16), vm((2, M // 2, width), BF16), vm((2, M // 2, width), F32),
                vm((2, M // 2, width), F32),
                vm((K, N, R, C), F32), vm((K, N, R, C), BF16), vm((K, N - 1, R, C), BF16),
                vm((K, R, C), BF16), vm((2, K, N - 1, R, C), BF16), vm((K, N, R, C), BF16),
                vm((K, N, TR, C), F32), vm((K, N, TR, C), T1), vm((K, N - 1, TR, C), T1),
                vm((K, TR, C), T2), vm((K, N - 1, TR, C), T2), vm((K, N, TR, C), TG),
                vm((M // 2, width), F32), vm((M // 2, width), BF16), vm((2, NZ - 1, M // 2, width), BF16),
                vm((8, 128), F32), vm((N * N - 1, 8, 128), F32),
                vm((probe_count, 8, 128), F32),
                dma((4,)), dma((K,)), dma((K,)), dma((1,)),
                dma((1,)), dma((K,)), dma((1,)), dma((3, K)), dma((1,)), dma((K,)), dma((1,)), dma((K,)),
                dma((3,)), dma((3,)),
                dma((1,)), dma((2,)),
                dma((1,)), dma((1,)),
            ],
            compiler_params=pltpu.CompilerParams(collective_id=0, has_side_effects=True),
        )(tokens, gain.reshape(1, width), gate_weight, up_weight, down_weight, probes)
        basis, stretch = pl.pallas_call(
            finish_kernel,
            out_shape=(
                jax.ShapeDtypeStruct(probes.shape, F32),
                jax.ShapeDtypeStruct((1, probe_count), F32),
            ),
            in_specs=[pl.BlockSpec(memory_space=pltpu.VMEM)] * 2,
            out_specs=(
                pl.BlockSpec(memory_space=pltpu.VMEM),
                pl.BlockSpec(memory_space=pltpu.VMEM),
            ),
        )(grown.reshape(probes.shape), level)
        return basis, stretch.reshape(probe_count)

    return jax.shard_map(
        local,
        mesh=torus,
        in_specs=(P(None, row), P(row), P(row, col), P(row, col), P(col, row), P(None, None, row)),
        out_specs=(P(None, None, row), P()),
        check_vma=False,
    )
```

```python
import functools

import jax
import jax.numpy as jnp
from jax import lax
from jax.experimental import pallas as pl
from jax.experimental.pallas import tpu as pltpu
from jax.sharding import Mesh
from jax.sharding import PartitionSpec as P

ITERS = 3
EPSILON = 1e-06
MESH = pl.DeviceIdType.MESH
F32 = jnp.float32
BF16 = jnp.bfloat16
NT = (((1,), (1,)), ((), ()))
CHUNK = 512
MODES = (3, 3, 3, 3, 3, 3, 3)
TOKEN_MODES = (3, 3, 3, 3, 3, 3, 3)
TOKEN_TYPES = (BF16, BF16, F32)
HOP = 3.0
STEP = 0.5


def stage_order(modes):
    events = []
    for k, mode in enumerate(modes):
        events.append((0.3 * k, 0, k))
        for stage in range(1, mode + 1):
            events.append((1.0 + STEP * (k + 1) + HOP * stage, stage, k))
    return [(stage, k) for _, stage, k in sorted(events)]


def kernel(
    cfg,
    tokens_hbm, gain_hbm, gate_hbm, up_hbm, down_hbm, probes_hbm,
    grown_hbm, level_ref,
    tokens_ref, gain_ref, probes_ref, gate_w, up_w, down_w,
    slope, act, pushed, tangent, grown_all, acc,
    joined, p1_src, p1_dst, p2_src, p2_dst, whole,
    t1_own, t1_src, t1_dst, t2_src, t2_dst, t_whole,
    pair_in, z_src, z_dst, sq, sq_in, scale,
    small_sem, gate_sem, up_sem, down_sem, p1_ss, p1_rs, p2_ss, p2_rs, g1_ss, g1_rs, g2_ss, g2_rs,
    pair_ss, pair_rs, z_ss, z_rs, sq_ss, sq_rs,
):
    N, NZ, K, C, probe_count, token_count, entries = cfg
    M = probe_count * token_count
    R = M // N
    W = C // N
    half = M // 2
    half_probes = probe_count // 2
    width = gain_ref.shape[1]
    x, y, z, c = (lax.axis_index(name) for name in ("x", "y", "z", "c"))
    other = 1 - c
    def around(v, n):
        return [v] + [lax.rem(v + d, n) for d in range(1, n)]

    xs, ys, zs = around(x, N), around(y, N), around(z, NZ)

    def device(i, j, k, core):
        return (i, j, k, core)

    a_at = (
        [xs[d] * other + ys[d] * c for d in range(N)],
        [ys[d] * other + xs[d] * c for d in range(N)],
    )
    a_devices = (
        [device(xs[d] * other + x * c, y * other + ys[d] * c, z, c) for d in range(N)],
        [device(xs[d] * c + x * other, y * c + ys[d] * other, z, c) for d in range(N)],
    )

    def a_of(k, d=0):
        return a_at[k % 2][d]

    def b_of(k, d=0):
        return a_at[1 - k % 2][d]

    def a_peer(k, d):
        return a_devices[k % 2][d]

    def b_peer(k, d):
        return a_devices[1 - k % 2][d]

    def row_peer(dx, dy):
        return device(xs[dx], ys[dy], z, c)

    z_peers = [device(x, y, zs[d], c) for d in range(NZ)]
    partner = device(x, y, z, other)
    row_offsets = [(dx, dy) for dx in range(N) for dy in range(N) if dx or dy]

    def columns(k):
        return slice(k * C, (k + 1) * C)

    def remote(src, dst, send, recv, target):
        return pltpu.make_async_remote_copy(
            src_ref=src, dst_ref=dst, send_sem=send, recv_sem=recv,
            device_id=target, device_id_type=MESH,
        )

    def wait_for(ref, sem):
        pltpu.make_async_copy(ref, ref, sem).wait()

    gate_loads = [
        pltpu.make_async_copy(gate_hbm.at[:, columns(k)], gate_w.at[:, columns(k)], gate_sem.at[k])
        for k in range(K)
    ]
    up_loads = [
        pltpu.make_async_copy(up_hbm.at[:, columns(k)], up_w.at[:, columns(k)], up_sem.at[k])
        for k in range(K)
    ]
    down_load = pltpu.make_async_copy(down_hbm, down_w, down_sem.at[0])
    tokens_load = pltpu.make_async_copy(tokens_hbm, tokens_ref, small_sem.at[0])
    gain_load = pltpu.make_async_copy(gain_hbm, gain_ref, small_sem.at[1])
    probes_load = pltpu.make_async_copy(probes_hbm, probes_ref, small_sem.at[2])
    tokens_load.start()
    gain_load.start()
    for k in range(K):
        gate_loads[k].start()
        up_loads[k].start()
    probes_load.start()
    down_load.start()

    barrier = pltpu.get_barrier_semaphore()
    greeted = [row_peer(dx, dy) for dx, dy in row_offsets]
    greeted += [z_peers[d] for d in range(1, NZ)] + [partner]
    for target in greeted:
        pl.semaphore_signal(barrier, inc=1, device_id=target, device_id_type=MESH)

    tokens_load.wait()
    gain_load.wait()
    gain = gain_ref[...]
    scaled = (tokens_ref[...].astype(F32) * gain).astype(BF16)

    far_first = sorted(range(1, N), key=lambda d: -min(d, N - d))
    near_first = far_first[::-1]

    def row_stages(phase, part, modes, src, dst, src2, dst2, gathered, consume, after_first=None):
        def block(j):
            return pl.ds(pl.multiple_of(j * W, W), W)

        def rs_a(k, d):
            return remote(src.at[k, a_of(k, d)], dst.at[k, d - 1], p1_ss.at[0], p1_rs.at[k], a_peer(k, d))

        def over_b(k, d):
            if modes[k] == 3:
                sent, taken = src2.at[k], dst2.at[k, d - 1]
            else:
                sent, taken = src2.at[k, :, block(b_of(k, d))], dst2.at[k, d - 1, :, 0:W]
            return remote(sent, taken, p2_ss.at[0], p2_rs.at[phase, k], b_peer(k, d))

        def ag_b(k, d):
            piece = gathered.at[k, a_of(k), :, block(b_of(k))]
            return remote(piece, piece, g1_ss.at[0], g1_rs.at[k], b_peer(k, d))

        def ag_a(k, d):
            piece = gathered.at[k, a_of(k)]
            return remote(piece, piece, g2_ss.at[0], g2_rs.at[k], a_peer(k, d))

        def first(k):
            part(k)
            for d in far_first:
                rs_a(k, d).start()

        kept = joined if src is p1_src else t1_own

        def second(k):
            wait_for(dst.at[k], p1_rs.at[k])
            total = kept[k, a_of(k)]
            for d in near_first:
                total += dst[k, d - 1].astype(F32)
            src2[k] = total.astype(src2.dtype)
            for d in far_first:
                over_b(k, d).start()
            kept[k, a_of(k)] = total

        def third(k):
            if modes[k] == 3:
                wait_for(dst2.at[k], p2_rs.at[phase, k])
                total = kept[k, a_of(k)]
                for d in near_first:
                    total += dst2[k, d - 1].astype(F32)
                gathered[k, a_of(k)] = total.astype(gathered.dtype)
                for d in far_first:
                    ag_a(k, d).start()
            else:
                wait_for(dst2.at[k, :, :, 0:W], p2_rs.at[phase, k])
                total = kept[k, a_of(k), :, block(b_of(k))]
                for d in near_first:
                    total += dst2[k, d - 1, :, 0:W].astype(F32)
                gathered[k, a_of(k), :, block(b_of(k))] = total.astype(gathered.dtype)
                for d in far_first:
                    ag_b(k, d).start()

        def fourth(k):
            wait_for(gathered.at[k, a_of(k), :, 0 : (N - 1) * W], g1_rs.at[k])
            for d in far_first:
                ag_a(k, d).start()

        def last(k):
            wait_for(gathered.at[k, 0 : N - 1], g2_rs.at[k])
            consume(k)

        def stages_of(k):
            return (first, second, third, last) if modes[k] == 3 else (first, second, third, fourth, last)

        wide = [k for k in range(K) if modes[k] == 3]
        narrow = [k for k in range(K) if modes[k] == 4]

        def finish():
            wait_for(dst, p1_ss.at[0])
            if narrow:
                wait_for(dst2.at[0 : len(narrow), :, :, 0:W], p2_ss.at[0])
                wait_for(gathered.at[0 : len(narrow), 0 : N - 1, :, 0:W], g1_ss.at[0])
            if wide:
                wait_for(dst2.at[0 : len(wide)], p2_ss.at[0])
            wait_for(gathered.at[:, 0 : N - 1], g2_ss.at[0])

        hook = after_first
        for stage, k in stage_order(modes):
            if stage and hook is not None:
                hook()
                hook = None
            stages_of(k)[stage](k)
        return finish

    halves = N // 2

    def token_compute(k):
        gate_loads[k].wait()
        up_loads[k].wait()
        gate = jnp.dot(scaled, gate_w[:, columns(k)], preferred_element_type=F32)
        up = jnp.dot(scaled, up_w[:, columns(k)], preferred_element_type=F32)
        gate = gate.reshape(halves, token_count // halves, C)
        up = up.reshape(halves, token_count // halves, C)
        t1_own[k, :halves] = gate
        t1_own[k, halves:] = up
        t1_src[k, :halves] = gate.astype(t1_src.dtype)
        t1_src[k, halves:] = up.astype(t1_src.dtype)

    for k in range(K):
        token_compute(k)
    pl.semaphore_wait(barrier, len(greeted))

    def token_use(k):
        gate = t_whole[k, :halves].reshape(token_count, C).astype(F32)
        up = t_whole[k, halves:].reshape(token_count, C).astype(F32)
        sigmoid = 1.0 / (1.0 + jnp.exp(-gate))
        act[:, columns(k)] = gate * sigmoid
        slope[:, columns(k)] = sigmoid * (1.0 + gate * (1.0 - sigmoid)) * up

    def start_probes():
        probes_load.wait()
        pushed[...] = (probes_ref[...] * gain[None]).astype(BF16).reshape(2, half, width)
        scale[...] = jnp.ones_like(scale)
        down_load.wait()

    row_stages(
        2, lambda k: None, TOKEN_MODES,
        t1_src, t1_dst, t2_src, t2_dst, t_whole, token_use, start_probes,
    )()

    def by_token(values, factor):
        return (values.reshape(probe_count, token_count, C) * factor[None]).reshape(M, C)

    def send_joined(k, value):
        blocks = value.reshape(N, R, C)
        joined[k] = blocks
        p1_src[k] = blocks.astype(BF16)

    def hidden_part(k):
        lhs = pushed[...].reshape(M, width)
        gate_tan = jnp.dot(lhs, gate_w[:, columns(k)], preferred_element_type=F32)
        up_tan = jnp.dot(lhs, up_w[:, columns(k)], preferred_element_type=F32)
        send_joined(k, by_token(gate_tan, slope[:, columns(k)]) + by_token(up_tan, act[:, columns(k)]))

    def add_to_acc(k, value):
        value = value.reshape(2, half, width)
        acc[...] = value if k == 0 else acc[...] + value

    def hidden_use(k):
        lhs = whole[k].reshape(M, C)
        add_to_acc(k, jnp.dot(lhs, down_w[columns(k), :], preferred_element_type=F32))

    def back_part(k):
        lhs = tangent[...].reshape(M, width)
        send_joined(k, lax.dot_general(lhs, down_w[columns(k), :], NT, preferred_element_type=F32))

    def back_use(k):
        piece = whole[k].reshape(M, C).astype(F32)
        gate_pull = by_token(piece, slope[:, columns(k)]).astype(BF16)
        up_pull = by_token(piece, act[:, columns(k)]).astype(BF16)
        value = lax.dot_general(gate_pull, gate_w[:, columns(k)], NT, preferred_element_type=F32)
        value += lax.dot_general(up_pull, up_w[:, columns(k)], NT, preferred_element_type=F32)
        add_to_acc(k, value)

    def col_half(phase, meanwhile):
        swap = remote(acc.at[other], pair_in, pair_ss.at[0], pair_rs.at[0], partner)
        swap.start()
        total = acc[c]
        swap.wait_recv()
        total += pair_in[...]
        z_src[...] = total.astype(z_src.dtype)
        copies = [
            remote(z_src, z_dst.at[phase, d - 1], z_ss.at[0], z_rs.at[phase], z_peers[d])
            for d in range(1, NZ)
        ]
        for d in sorted(range(1, NZ), key=lambda d: -min(d, NZ - d)):
            copies[d - 1].start()
        acc[c] = total
        swap.wait_send()
        meanwhile()
        wait_for(z_dst.at[phase], z_rs.at[phase])
        total = acc[c]
        for d in range(1, NZ):
            total += z_dst[phase, d - 1].astype(F32)
        wait_for(z_dst.at[phase], z_ss.at[0])
        return total

    def share(buffer, which):
        mine, theirs = buffer.at[c], buffer.at[other]
        send, recv = pair_ss.at[which], pair_rs.at[which]
        remote(mine, mine, send, recv, partner).start()
        remote(theirs, theirs, send, recv, partner).wait_recv()
        remote(mine, mine, send, recv, partner).wait_send()

    def folded(values):
        rows, lanes = values.shape
        total = None
        for r in range(0, rows, 8):
            for l in range(0, lanes, 128):
                piece = values[r : r + 8, l : l + 128]
                total = piece if total is None else total + piece
        return jnp.sum(total, axis=0, keepdims=True)

    def square_copies():
        return [
            remote(sq, sq_in.at[slot], sq_ss.at[0], sq_rs.at[0], row_peer(dx, dy))
            for slot, (dx, dy) in enumerate(row_offsets)
        ]

    def send_squares():
        for p in range(probe_count):
            i, j = divmod(p, half_probes)
            values = grown_all[i, j * token_count : (j + 1) * token_count]
            sq[p : p + 1] = folded(values * values)
        for cp in square_copies():
            cp.start()

    def levels():
        total = sq[...]
        wait_for(sq_in, sq_rs.at[0])
        for slot in range(len(row_offsets)):
            total += sq_in[slot]
        wait_for(sq_in, sq_ss.at[0])
        return jnp.sum(total, axis=1, keepdims=True) / entries

    def sweep(it, carry):
        def squares():
            @pl.when(it > 0)
            def _():
                send_squares()

        finish = row_stages(
            0, hidden_part, MODES,
            p1_src, p1_dst, p2_src, p2_dst.at[0], whole, hidden_use, squares,
        )

        def meanwhile():
            finish()

            @pl.when(it > 0)
            def _():
                factor = lax.rsqrt(levels() + EPSILON)
                for p in range(probe_count):
                    scale[p] = jnp.broadcast_to(factor[p : p + 1], scale.shape[1:])

        total = col_half(0, meanwhile)
        parts = [
            total[i * token_count : (i + 1) * token_count] * scale[c * half_probes + i, 0:1, 0:1]
            for i in range(half_probes)
        ]
        tangent[c] = jnp.concatenate(parts, axis=0).astype(BF16)
        share(tangent, 1)

        finish = row_stages(
            1, back_part, MODES,
            p1_src, p1_dst, p2_src, p2_dst.at[1], whole, back_use,
        )
        grown_all[c] = col_half(1, finish) * gain
        share(grown_all, 2)
        pushed[...] = (grown_all[...] * gain[None]).astype(BF16)
        return carry

    sq[...] = jnp.zeros_like(sq)
    lax.fori_loop(0, ITERS, sweep, 0)

    send_squares()
    out = pltpu.make_async_copy(grown_all, grown_hbm, small_sem.at[3])
    out.start()
    level_ref[...] = jnp.broadcast_to(levels(), level_ref.shape)
    out.wait()


def finish_kernel(grown_ref, level_ref, basis_ref, stretch_ref):
    probe_count = basis_ref.shape[0]
    level = level_ref[...]
    root = jnp.sqrt(level)
    factor = lax.rsqrt(level + EPSILON)
    lane = lax.broadcasted_iota(jnp.int32, (1, probe_count), 1)
    stretch = jnp.zeros((1, probe_count), F32)
    for p in range(probe_count):
        stretch = jnp.where(lane == p, root[p : p + 1, 0:1], stretch)
        basis_ref[p] = grown_ref[p] * factor[p : p + 1, 0:1]
    stretch_ref[...] = stretch


def solution(mesh, chunk=CHUNK, shape=(4, 4, 4, 2)):
    N, _, NZ, _ = shape
    torus = Mesh(mesh.devices.reshape(shape), ("x", "y", "z", "c"))
    row, col = ("x", "y"), ("z", "c")

    def local(tokens, gain, gate_weight, up_weight, down_weight, probes):
        probe_count, token_count, width = probes.shape
        hidden = gate_weight.shape[1]
        M = probe_count * token_count
        K, C = hidden // chunk, chunk
        R = M // N
        TR = 2 * token_count // N
        T1, T2, TG = TOKEN_TYPES
        entries = token_count * width * N * N
        cfg = (N, NZ, K, C, probe_count, token_count, entries)
        vm = pltpu.VMEM
        dma = pltpu.SemaphoreType.DMA
        grown, level = pl.pallas_call(
            functools.partial(kernel, cfg),
            out_shape=(
                jax.ShapeDtypeStruct((2, M // 2, width), F32),
                jax.ShapeDtypeStruct((8, 128), F32),
            ),
            in_specs=[pl.BlockSpec(memory_space=pl.ANY)] * 6,
            out_specs=(
                pl.BlockSpec(memory_space=pl.ANY),
                pl.BlockSpec(memory_space=pltpu.VMEM),
            ),
            scratch_shapes=[
                vm((token_count, width), BF16), vm((1, width), F32), vm(probes.shape, F32),
                vm((width, hidden), BF16), vm((width, hidden), BF16), vm((hidden, width), BF16),
                vm((token_count, hidden), F32), vm((token_count, hidden), F32),
                vm((2, M // 2, width), BF16), vm((2, M // 2, width), BF16), vm((2, M // 2, width), F32),
                vm((2, M // 2, width), F32),
                vm((K, N, R, C), F32), vm((K, N, R, C), BF16), vm((K, N - 1, R, C), BF16),
                vm((K, R, C), BF16), vm((2, K, N - 1, R, C), BF16), vm((K, N, R, C), BF16),
                vm((K, N, TR, C), F32), vm((K, N, TR, C), T1), vm((K, N - 1, TR, C), T1),
                vm((K, TR, C), T2), vm((K, N - 1, TR, C), T2), vm((K, N, TR, C), TG),
                vm((M // 2, width), F32), vm((M // 2, width), BF16), vm((2, NZ - 1, M // 2, width), BF16),
                vm((8, 128), F32), vm((N * N - 1, 8, 128), F32),
                vm((probe_count, 8, 128), F32),
                dma((4,)), dma((K,)), dma((K,)), dma((1,)),
                dma((1,)), dma((K,)), dma((1,)), dma((3, K)), dma((1,)), dma((K,)), dma((1,)), dma((K,)),
                dma((3,)), dma((3,)),
                dma((1,)), dma((2,)),
                dma((1,)), dma((1,)),
            ],
            compiler_params=pltpu.CompilerParams(collective_id=0, has_side_effects=True),
        )(tokens, gain.reshape(1, width), gate_weight, up_weight, down_weight, probes)
        basis, stretch = pl.pallas_call(
            finish_kernel,
            out_shape=(
                jax.ShapeDtypeStruct(probes.shape, F32),
                jax.ShapeDtypeStruct((1, probe_count), F32),
            ),
            in_specs=[pl.BlockSpec(memory_space=pltpu.VMEM)] * 2,
            out_specs=(
                pl.BlockSpec(memory_space=pltpu.VMEM),
                pl.BlockSpec(memory_space=pltpu.VMEM),
            ),
        )(grown.reshape(probes.shape), level)
        return basis, stretch.reshape(probe_count)

    return jax.shard_map(
        local,
        mesh=torus,
        in_specs=(P(None, row), P(row), P(row, col), P(row, col), P(col, row), P(None, None, row)),
        out_specs=(P(None, None, row), P()),
        check_vma=False,
    )
```
